128 devices in a mesh: own: 32 (over x, z, core), rep: 4 (over y).
Axes of the slice: x: 4, y: 4, z: 4, core: 2. Of those that a mesh axis runs over, the one named last changes fastest.
Arguments:
- block_pool: bfloat16 [8192, 64, 576], P(('own', 'rep')), may hold values from -16 to 16
- sel_index: int32 [4096], P(('own', 'rep')), may hold values from 0 to 63
- sel_layer: int32 [4096], P(('own', 'rep')), may hold values from 0 to 15, as said below
- counts: int32 [128], P(('own', 'rep')), may hold values from 8 to 32, as said below
Outputs:
- quant_codes: bfloat16 [32, 4, 32, 8, 18432], P('own', 'rep')
- quant_steps: float32 [32, 288], P('own')
- clip_error: float32 [32, 288], P('own')
The draws below stay inside these ranges and needn't reach their ends.
Inputs may be any that keep to these rules, and one draw needn't show every extreme that they name: `sel_layer`: among the 32 entries of one device, at most 8 name any one layer; the first 8 entries of every device all name one and the same layer. `counts`: some device has all 32 entries live.
All inputs are finite; a program needn't handle non-finite values.
Results may differ from the reference program's by a relative error of at most 0.001.
Values may be sent and summed in bfloat16 or wider, within the bound.
No kernel may reach another device: no remote copies, remote signals or barrier semaphores. Data moves between devices by JAX's collectives and lax.ppermute only.
A program may use at most 128 MiB of HBM per device.

```python
import math
import jax
import jax.numpy as jnp
from jax import lax

LATENT = 576
TOKB = 64
SLICES = 2
CAP = 8
POOL_DEV = 64
SEL_DEV = 32
LAYERS = 16
HALF = 288
SEL_ALL = 4096
N_OWN = 32
N_REP = 4


def draw_block_pool(key, part):
    base_key = jax.random.fold_in(key, 11)
    key_chan, key_base, key_rows = jax.random.split(base_key, 3)
    shape = (N_OWN * N_REP * POOL_DEV, TOKB, LATENT)
    channel = jnp.exp(jax.random.uniform(key_chan, (LATENT,), jnp.float32, math.log(0.3), math.log(3.0)))
    base = jnp.clip(jax.random.normal(key_base, shape, jnp.float32), -5.0, 5.0)
    row_scale = jnp.ones((shape[0], 1, 1), jnp.float32)
    return (base * channel * row_scale).astype(jnp.bfloat16)


def draw_sel_layer(key, part):
    devices = N_OWN * N_REP
    base_key = jax.random.fold_in(key, 31)
    key_star, key_perm = jax.random.split(base_key, 2)
    star_layer = jax.random.randint(key_star, (), 0, LAYERS)
    items = jnp.arange((LAYERS - 1) * CAP, dtype=jnp.int32) // CAP
    device_keys = jax.random.split(key_perm, devices)

    def per_device(device_key):
        shuffled = jax.random.permutation(device_key, items)[:SEL_DEV - CAP]
        others = (star_layer + 1 + shuffled) % LAYERS
        front = jnp.full((CAP,), star_layer, jnp.int32)
        return jnp.concatenate([front, others.astype(jnp.int32)])
    return jax.vmap(per_device)(device_keys).reshape(-1).astype(jnp.int32)


def draw_counts(key, part):
    devices = N_OWN * N_REP
    base_key = jax.random.fold_in(key, 21)
    key_low, key_full, key_first = jax.random.split(base_key, 3)
    lower = jax.random.randint(key_low, (devices,), CAP, CAP + (SEL_DEV - CAP) // 3 + 1)
    full_mask = jax.random.randint(key_full, (devices,), 0, 8) == 0
    first_full = jax.random.randint(key_first, (), 0, devices)
    full_mask = full_mask | (jnp.arange(devices) == first_full)
    return jnp.where(full_mask, SEL_DEV, lower).astype(jnp.int32)


def touch_ends(drawn, stream_key, low, high):
    index_at = [jax.random.randint(jax.random.fold_in(stream_key, axis), (), 0, length) for axis, length in enumerate(drawn.shape)]
    main_axis = drawn.shape.index(max(drawn.shape))
    neighbour = index_at[:main_axis] + [(index_at[main_axis] + 1) % drawn.shape[main_axis]] + index_at[main_axis + 1:]
    return drawn.at[tuple(index_at)].set(low).at[tuple(neighbour)].set(high)


def setup_inputs(seed: int = 0) -> dict:
    seeds = jax.random.split(jax.random.key(seed), 5)
    return {
        "block_pool": draw_block_pool(jax.random.fold_in(seeds[4], 71), 0),
        "sel_index": touch_ends(jax.random.randint(seeds[1], (SEL_ALL,), 0, POOL_DEV), jax.random.fold_in(seeds[1], 1), 0, POOL_DEV - 1).astype(jnp.int32),
        "sel_layer": draw_sel_layer(jax.random.fold_in(seeds[4], 71), 0),
        "counts": draw_counts(jax.random.fold_in(seeds[4], 71), 0),
    }


headroom = 0.5


def slot_table(index_row, layer_row, live_count, group_layer, capacity):
    n_select = index_row.shape[0]
    is_live = jnp.arange(n_select) < live_count
    matches = (layer_row[None, :] == group_layer[:, None]) & is_live[None, :]
    ranking = jnp.cumsum(matches.astype(jnp.int32), axis=1) - 1
    slot_hit = matches[:, None, :] & (ranking[:, None, :] == jnp.arange(capacity)[None, :, None])
    chosen = jnp.sum(jnp.where(slot_hit, index_row[None, None, :], 0), axis=2).astype(jnp.int32)
    filled = jnp.any(slot_hit, axis=2)
    return chosen, filled


def reference(block_pool, sel_index, sel_layer, counts):
    devices = N_OWN * N_REP
    group_layer = (jnp.arange(N_OWN) // SLICES).astype(jnp.int32)
    index_rows = sel_index.reshape(devices, SEL_DEV)
    layer_rows = sel_layer.reshape(devices, SEL_DEV)
    chosen, filled = jax.vmap(lambda a, b, c: slot_table(a, b, c, group_layer, CAP))(index_rows, layer_rows, counts)
    pools = block_pool.reshape(devices, POOL_DEV, TOKB, SLICES, HALF)
    device_ids = jnp.arange(devices)[:, None]
    denominator = float(N_OWN * N_REP * CAP * TOKB)

    def one_group(group):
        slice_of = group % SLICES
        picked = jnp.take(chosen, group, axis=1)
        keep_mask = jnp.take(filled, group, axis=1)
        blocks = pools[device_ids, picked, :, slice_of]
        blocks = jnp.where(keep_mask[:, :, None, None], blocks, jnp.zeros((), blocks.dtype))
        values = blocks.astype(jnp.float32)
        peak_abs = jnp.max(jnp.abs(values), axis=(0, 1, 2))
        step_size = headroom * jnp.maximum(peak_abs, 1.0) / 127.0
        encoded = jnp.clip(values / step_size, -127.0, 127.0).astype(jnp.bfloat16)
        encoded = lax.optimization_barrier(encoded)
        decoded = encoded.astype(jnp.float32) * step_size
        sq_error = jnp.sum((values - decoded) ** 2, axis=(0, 1, 2))
        error_out = sq_error / (step_size * step_size * denominator)
        codes_out = encoded.reshape(N_OWN, N_REP, CAP, TOKB * HALF).transpose(1, 0, 2, 3)
        return codes_out, step_size, error_out

    quant_codes, quant_steps, clip_error = lax.map(one_group, jnp.arange(N_OWN))
    return quant_codes, quant_steps, clip_error
```

```python
import functools
import jax
import jax.numpy as jnp
from jax import lax
from jax.experimental import pallas as pl
from jax.experimental.pallas import tpu as pltpu
from jax.sharding import PartitionSpec as P

SLICES = 2
CAP = 8
LANES = 128
PITCH = 72
headroom = 0.5


def peak_kernel(layers, index_ref, layer_ref, count_ref, pool_ref, peak_ref, held, acc, sems):
    live = count_ref[0]

    def fetch(j):
        return pltpu.make_async_copy(pool_ref.at[index_ref[j]], held.at[j], sems.at[j])

    def start(j, carry):
        fetch(j).start()
        return carry

    lax.fori_loop(0, live, start, 0)
    acc[...] = jnp.zeros_like(acc)

    def one(j, carry):
        fetch(j).wait()
        layer = layer_ref[j]
        tokens, width = held.shape[1:]
        values = jnp.abs(held[j].astype(jnp.float32)).reshape(tokens // 8, 8, width)
        acc[layer] = jnp.maximum(acc[layer], jnp.max(values, axis=0))
        return carry

    lax.fori_loop(0, live, one, 0)
    peak_ref[...] = jnp.max(acc[...], axis=1)


def encode_kernel(
    layers, index_ref, layer_ref, count_ref, me_ref, pool_ref, peak_ref,
    codes_ref, error_ref, steps_ref, held, spread, slots, filled, sems,
):
    step = pl.program_id(0)
    live = count_ref[0]
    tokens, width = held.shape[1:]
    half = width // SLICES
    tiles = spread.shape[0]

    def fetch(j):
        return pltpu.make_async_copy(pool_ref.at[index_ref[j]], held.at[j], sems.at[j])

    @pl.when(step == 0)
    def _():
        def clear(layer, carry):
            filled[layer] = 0
            return carry

        lax.fori_loop(0, layers, clear, 0)

        def start(j, carry):
            fetch(j).start()
            layer = layer_ref[j]
            at = filled[layer]
            slots[layer * CAP + at] = j
            filled[layer] = at + 1
            return carry

        lax.fori_loop(0, live, start, 0)

        def wait(j, carry):
            fetch(j).wait()
            return carry

        lax.fori_loop(0, live, wait, 0)
        own = peak_ref[pl.ds(me_ref[0] // SLICES, 1), :]
        own = jnp.where(me_ref[0] % SLICES == 0, own[:, :half], own[:, half:])
        steps_ref[...] = headroom * jnp.maximum(own, 1.0) / 127.0

    held_slots = filled[step]
    scale = headroom * jnp.maximum(peak_ref[pl.ds(step, 1), :], 1.0) / 127.0

    @pl.when(held_slots == 0)
    def _():
        codes_ref[...] = jnp.zeros_like(codes_ref)
        error_ref[...] = jnp.zeros_like(error_ref)

    @pl.when(held_slots > 0)
    def _():
        def code(c, total):
            values = held[slots[step * CAP + c]].astype(jnp.float32)
            coded = jnp.clip(values / scale, -127.0, 127.0).astype(jnp.bfloat16).astype(jnp.float32)
            rows = pl.ds(pl.multiple_of(c * PITCH, 8), tokens)
            for j in range(tiles):
                lanes = min(LANES, width - j * LANES)
                spread[j, rows, :lanes] = coded[:, j * LANES : j * LANES + lanes]
            miss = values - coded * scale
            return total + jnp.sum((miss * miss).reshape(tokens // 8, 8, width), axis=0)

        total = lax.fori_loop(0, held_slots, code, jnp.zeros((8, width), jnp.float32))
        error_ref[0] = jnp.sum(total, axis=0, keepdims=True)

        def blank(c, carry):
            for j in range(tiles):
                spread[j, pl.ds(pl.multiple_of(c * PITCH, 8), tokens), :] = jnp.zeros((tokens, LANES), jnp.float32)
            return carry

        lax.fori_loop(held_slots, CAP, blank, 0)

        lane = lax.broadcasted_iota(jnp.int32, (CAP, LANES), 1)
        group = 4 * half

        def four_tokens(u, carry):
            rows = [
                [spread[j, pl.ds(4 * u + q, CAP, stride=PITCH), :] for j in range(tiles)]
                for q in range(4)
            ]
            for h in range(SLICES):
                turned = {}
                for i in range(group // LANES):
                    out, at = None, 0
                    while at < LANES:
                        flat = i * LANES + at
                        q = flat // half
                        source = flat - q * half + h * half
                        j = source // LANES
                        run = min(LANES - source % LANES, (q + 1) * half - flat, LANES - at)
                        if (q, j) not in turned:
                            shift = (at - source) % LANES
                            turned[q, j] = pltpu.roll(rows[q][j], shift, 1) if shift else rows[q][j]
                        piece = turned[q, j]
                        out = piece if out is None else jnp.where(lane >= at, piece, out)
                        at += run
                    place = pl.ds(pl.multiple_of(u * group + i * LANES, LANES), LANES)
                    codes_ref[h, :, place] = out.astype(jnp.bfloat16)
            return carry

        lax.fori_loop(0, tokens // 4, four_tokens, 0)


def local_peaks(block_pool, sel_index, sel_layer, counts, layers):
    n_select = sel_index.shape[0]
    tokens, width = block_pool.shape[1:]
    smem = pl.BlockSpec(memory_space=pltpu.SMEM)
    return pl.pallas_call(
        functools.partial(peak_kernel, layers),
        out_shape=jax.ShapeDtypeStruct((layers, width), jnp.float32),
        in_specs=[smem, smem, smem, pl.BlockSpec(memory_space=pl.ANY)],
        out_specs=pl.BlockSpec(memory_space=pltpu.VMEM),
        scratch_shapes=[
            pltpu.VMEM((n_select, tokens, width), jnp.bfloat16),
            pltpu.VMEM((layers, 8, width), jnp.float32),
            pltpu.SemaphoreType.DMA((n_select,)),
        ],
        name="peaks",
    )(sel_index, sel_layer, counts, block_pool)


def encode(block_pool, sel_index, sel_layer, counts, me, peak, layers):
    n_select = sel_index.shape[0]
    tokens, width = block_pool.shape[1:]
    half = width // SLICES
    tiles = pl.cdiv(width, LANES)
    smem = pl.BlockSpec(memory_space=pltpu.SMEM)
    return pl.pallas_call(
        functools.partial(encode_kernel, layers),
        grid=(layers,),
        out_shape=(
            jax.ShapeDtypeStruct((layers * SLICES, CAP, tokens * half), jnp.bfloat16),
            jax.ShapeDtypeStruct((layers, 1, width), jnp.float32),
            jax.ShapeDtypeStruct((1, half), jnp.float32),
        ),
        in_specs=[smem, smem, smem, smem, pl.BlockSpec(memory_space=pl.ANY), pl.BlockSpec((layers, width), lambda l: (0, 0))],
        out_specs=(
            pl.BlockSpec((SLICES, CAP, tokens * half), lambda l: (l, 0, 0)),
            pl.BlockSpec((1, 1, width), lambda l: (l, 0, 0)),
            pl.BlockSpec((1, half), lambda l: (0, 0)),
        ),
        scratch_shapes=[
            pltpu.VMEM((n_select, tokens, width), jnp.bfloat16),
            pltpu.VMEM((tiles, CAP * PITCH, LANES), jnp.float32),
            pltpu.SMEM((layers * CAP,), jnp.int32),
            pltpu.SMEM((layers,), jnp.int32),
            pltpu.SemaphoreType.DMA((n_select,)),
        ],
        name="encode",
    )(sel_index, sel_layer, counts, me, block_pool, peak)


def body(block_pool, sel_index, sel_layer, counts):
    own_count = lax.axis_size("own")
    rep_count = lax.axis_size("rep")
    layers = own_count // SLICES
    tokens, width = block_pool.shape[1:]
    me = lax.axis_index("own").astype(jnp.int32)
    peak = local_peaks(block_pool, sel_index, sel_layer, counts, layers)
    peak = lax.pmax(peak, ("own", "rep"))
    codes, error, steps = encode(block_pool, sel_index, sel_layer, counts, me[None], peak, layers)
    arrived = lax.all_to_all(codes, "own", split_axis=0, concat_axis=0, tiled=True)
    total = lax.psum(error, ("own", "rep")).reshape(own_count, width // SLICES)
    mine = lax.dynamic_slice_in_dim(total, me, 1, axis=0)
    denominator = float(own_count * rep_count * CAP * tokens)
    return arrived[None, None], steps, mine / (steps * steps * denominator)


def solution(mesh):
    return jax.shard_map(
        body,
        mesh=mesh,
        in_specs=(
            P(("own", "rep"), None, None),
            P(("own", "rep")),
            P(("own", "rep")),
            P(("own", "rep")),
        ),
        out_specs=(P("own", "rep", None, None, None), P("own", None), P("own", None)),
        check_vma=False,
    )
```

```python
import functools
import jax
import jax.numpy as jnp
from jax import lax
from jax.experimental import pallas as pl
from jax.experimental.pallas import tpu as pltpu
from jax.sharding import PartitionSpec as P

SLICES = 2
CAP = 8
LANES = 128
QUAD = 4
CHUNKS = (4, 8, 4)
headroom = 0.5


def round_up(n, to):
    return -(-n // to) * to


def lay_out_kernel(
    layers, firsts, counts, peaks, index_ref, layer_ref, count_ref, pool_ref, *refs
):
    outs, (held, spread, slots, filled, sems, *acc) = refs[: len(firsts)], refs[len(firsts) :]
    step = pl.program_id(0)
    live = count_ref[0]
    tokens, width = held.shape[1:]
    half = width // SLICES
    tiles = spread.shape[0]
    pitch = spread.shape[1] // CAP
    group = QUAD * half
    first_token, last_token = QUAD * firsts[0], QUAD * (firsts[-1] + counts[-1])
    here = last_token - first_token

    def fetch(j):
        return pltpu.make_async_copy(pool_ref.at[index_ref[j]], held.at[j], sems.at[j])

    @pl.when(step == 0)
    def _():
        def clear(layer, carry):
            filled[layer] = 0
            return carry

        lax.fori_loop(0, layers, clear, 0)

        def start(j, carry):
            fetch(j).start()
            layer = layer_ref[j]
            at = filled[layer]
            slots[layer * CAP + at] = j
            filled[layer] = at + 1
            return carry

        lax.fori_loop(0, live, start, 0)
        if peaks:
            acc[0][...] = jnp.zeros_like(acc[0])

        def wait(j, carry):
            fetch(j).wait()
            if peaks:
                layer = layer_ref[j]
                values = jnp.abs(held[j].astype(jnp.float32)).reshape(tokens // 8, 8, width)
                acc[0][layer] = jnp.maximum(acc[0][layer], jnp.max(values, axis=0))
            return carry

        lax.fori_loop(0, live, wait, 0)

    held_slots = filled[step]

    @pl.when(held_slots == 0)
    def _():
        for out in outs:
            out[...] = jnp.zeros_like(out)

    @pl.when(held_slots > 0)
    def _():
        def place(c, carry):
            values = held[slots[step * CAP + c], first_token:last_token, :].astype(jnp.float32)
            rows = pl.ds(pl.multiple_of(c * pitch, 8), here)
            for j in range(tiles):
                lanes = min(LANES, width - j * LANES)
                spread[j, rows, :lanes] = values[:, j * LANES : j * LANES + lanes]
            return carry

        lax.fori_loop(0, held_slots, place, 0)

        def blank(c, carry):
            for j in range(tiles):
                spread[j, pl.ds(pl.multiple_of(c * pitch, 8), here), :] = jnp.zeros((here, LANES), jnp.float32)
            return carry

        lax.fori_loop(held_slots, CAP, blank, 0)

        lane = lax.broadcasted_iota(jnp.int32, (CAP, LANES), 1)
        if peaks:
            end = counts[0] * group
            outs[0][:, :, end:] = jnp.zeros((SLICES, CAP, outs[0].shape[2] - end), jnp.bfloat16)
            top = jnp.max(acc[0][step], axis=0, keepdims=True)
            for h in range(SLICES):
                one = jnp.broadcast_to(top[:, h * half : (h + 1) * half], (CAP, half))
                outs[0][h, :, end : end + half] = one.astype(jnp.bfloat16)

        for out, first, count in zip(outs, firsts, counts):

            def four_tokens(u, carry, out=out, first=first):
                at_row = QUAD * (u + first) - first_token
                rows = [
                    [spread[j, pl.ds(at_row + q, CAP, stride=pitch), :] for j in range(tiles)]
                    for q in range(QUAD)
                ]
                for h in range(SLICES):
                    turned = {}
                    for i in range(group // LANES):
                        whole, at = None, 0
                        while at < LANES:
                            flat = i * LANES + at
                            q = flat // half
                            source = flat - q * half + h * half
                            j = source // LANES
                            run = min(LANES - source % LANES, (q + 1) * half - flat, LANES - at)
                            if (q, j) not in turned:
                                shift = (at - source) % LANES
                                turned[q, j] = pltpu.roll(rows[q][j], shift, 1) if shift else rows[q][j]
                            piece = turned[q, j]
                            whole = piece if whole is None else jnp.where(lane >= at, piece, whole)
                            at += run
                        where = pl.ds(pl.multiple_of(u * group + i * LANES, LANES), LANES)
                        out[h, :, where] = whole.astype(jnp.bfloat16)
                return carry

            lax.fori_loop(0, count, four_tokens, 0)


def lay_out(block_pool, sel_index, sel_layer, counts, layers, firsts, groups, peaks, after=()):
    n_select = sel_index.shape[0]
    tokens, width = block_pool.shape[1:]
    half = width // SLICES
    tiles = pl.cdiv(width, LANES)
    here = QUAD * sum(groups)
    pitch = here + 8
    smem = pl.BlockSpec(memory_space=pltpu.SMEM)
    sizes = [QUAD * half * n for n in groups]
    if peaks:
        sizes[0] += round_up(half, LANES)
    scratch = [
        pltpu.VMEM((n_select, tokens, width), jnp.bfloat16),
        pltpu.VMEM((tiles, CAP * pitch, LANES), jnp.float32),
        pltpu.SMEM((layers * CAP,), jnp.int32),
        pltpu.SMEM((layers,), jnp.int32),
        pltpu.SemaphoreType.DMA((n_select,)),
    ]
    if peaks:
        scratch.append(pltpu.VMEM((layers, 8, width), jnp.float32))
    return pl.pallas_call(
        functools.partial(lay_out_kernel, layers, firsts, groups, peaks),
        grid=(layers,),
        out_shape=[jax.ShapeDtypeStruct((layers * SLICES, CAP, n), jnp.bfloat16) for n in sizes],
        in_specs=[smem, smem, smem, pl.BlockSpec(memory_space=pl.ANY)],
        out_specs=[pl.BlockSpec((SLICES, CAP, n), lambda l: (l, 0, 0)) for n in sizes],
        scratch_shapes=scratch,
        cost_estimate=pl.CostEstimate(flops=100_000_000, bytes_accessed=20_000_000, transcendentals=0),
        name="lay_out",
    )(sel_index, sel_layer, counts, block_pool)


def encode_kernel(step_ref, inverse_ref, error_in, raw_ref, *refs):
    codes_ref, error_ref = refs[-2:]

    @pl.when(pl.program_id(0) == 0)
    def _():
        error_ref[...] = error_in[...]

    sources, cap, lanes = raw_ref.shape
    tiles = lanes // LANES
    step = [jnp.broadcast_to(step_ref[:, i * LANES : (i + 1) * LANES], (cap, LANES)) for i in range(tiles)]
    inverse = [jnp.broadcast_to(inverse_ref[:, i * LANES : (i + 1) * LANES], (cap, LANES)) for i in range(tiles)]

    def source(s, totals):
        out = []
        for i in range(tiles):
            at = slice(i * LANES, (i + 1) * LANES)
            values = raw_ref[s, :, at].astype(jnp.float32)
            coded = jnp.clip(values * inverse[i], -127.0, 127.0).astype(jnp.bfloat16)
            codes_ref[s, :, at] = coded
            miss = values - coded.astype(jnp.float32) * step[i]
            out.append(totals[i] + miss * miss)
        return tuple(out)

    zeros = tuple(jnp.zeros((cap, LANES), jnp.float32) for _ in range(tiles))
    totals = lax.fori_loop(0, sources, source, zeros)
    for i in range(tiles):
        error_ref[:, i * LANES : (i + 1) * LANES] += totals[i]


def encode(raw, step_row, inverse_row, error, codes, first, groups, all_groups):
    sources, cap, _ = raw.shape
    lanes = step_row.shape[1]
    row = pl.BlockSpec((1, lanes), lambda u: (0, 0))
    total = pl.BlockSpec((cap, lanes), lambda u: (0, 0))
    specs = [row, row, total, pl.BlockSpec((sources, cap, lanes), lambda u: (0, 0, u))]
    args = [step_row, inverse_row, error, raw]
    aliases = {}
    if codes is not None:
        specs.append(pl.BlockSpec(memory_space=pl.ANY))
        args.append(codes)
        aliases = {4: 0}
    return pl.pallas_call(
        encode_kernel,
        grid=(groups,),
        out_shape=(
            jax.ShapeDtypeStruct((sources, cap, lanes * all_groups), jnp.bfloat16),
            jax.ShapeDtypeStruct((cap, lanes), jnp.float32),
        ),
        in_specs=specs,
        out_specs=(pl.BlockSpec((sources, cap, lanes), lambda u: (0, 0, first + u)), total),
        input_output_aliases=aliases,
        cost_estimate=pl.CostEstimate(flops=20_000_000 * groups, bytes_accessed=1_200_000 * groups, transcendentals=0),
        name="encode",
    )(*args)


def over_rep(x, op):
    x = op(x, lax.ppermute(x, "rep", [(0, 1), (1, 0), (2, 3), (3, 2)]))
    return op(x, lax.ppermute(x, "rep", [(0, 3), (3, 0), (1, 2), (2, 1)]))


def body(block_pool, sel_index, sel_layer, counts):
    own_count = lax.axis_size("own")
    rep_count = lax.axis_size("rep")
    layers = own_count // SLICES
    tokens, width = block_pool.shape[1:]
    half = width // SLICES
    firsts = [sum(CHUNKS[:n]) for n in range(len(CHUNKS))]

    def exchange(x):
        return lax.all_to_all(x, "own", split_axis=0, concat_axis=0, tiled=True)

    sent = lay_out(block_pool, sel_index, sel_layer, counts, layers, firsts[:1], CHUNKS[:1], True)
    sent += lay_out(block_pool, sel_index, sel_layer, counts, layers, firsts[1:], CHUNKS[1:], False)
    arrived = [exchange(x) for x in sent]

    at = QUAD * half * CHUNKS[0]
    peak = jnp.max(arrived[0][:, :1, at : at + half], axis=0).astype(jnp.float32)
    peak = over_rep(peak, jnp.maximum)
    steps = headroom * jnp.maximum(peak, 1.0) / 127.0
    step_row = jnp.tile(steps, (1, QUAD))
    inverse_row = 1.0 / step_row
    error = jnp.zeros((CAP, QUAD * half), jnp.float32)
    codes = None
    for n, raw in enumerate(arrived):
        codes, error = encode(
            raw, step_row, inverse_row, error, codes, firsts[n], CHUNKS[n], tokens // QUAD
        )
    error = jnp.sum(jnp.sum(error, axis=0).reshape(QUAD, half), axis=0, keepdims=True)
    error = over_rep(error, jnp.add)
    denominator = float(own_count * rep_count * CAP * tokens)
    return codes[None, None], steps, error / (steps * steps * denominator)


def solution(mesh):
    return jax.shard_map(
        body,
        mesh=mesh,
        in_specs=(
            P(("own", "rep"), None, None),
            P(("own", "rep")),
            P(("own", "rep")),
            P(("own", "rep")),
        ),
        out_specs=(P("own", "rep", None, None, None), P("own", None), P("own", None)),
        check_vma=False,
    )
```

```python
import functools
import jax
import jax.numpy as jnp
from jax import lax
from jax.experimental import pallas as pl
from jax.experimental.pallas import tpu as pltpu
from jax.sharding import PartitionSpec as P

SLICES = 2
CAP = 8
LANES = 128
QUAD = 4
CHUNKS = (4, 12)
headroom = 0.5


def round_up(n, to):
    return -(-n // to) * to


def lay_out_kernel(
    layers, firsts, counts, peaks, index_ref, layer_ref, count_ref, pool_ref, *refs
):
    outs, (held, spread, slots, filled, dirty, sems, *tops) = refs[: len(firsts)], refs[len(firsts) :]
    step = pl.program_id(0)
    live = count_ref[0]
    tokens, width = held.shape[1:]
    half = width // SLICES
    tiles = spread.shape[0]
    pitch = spread.shape[1] // CAP
    group = QUAD * half
    first_token, last_token = QUAD * firsts[0], QUAD * (firsts[-1] + counts[-1])
    here = last_token - first_token
    pieces = pl.cdiv(half, LANES)

    def fetch(j):
        return pltpu.make_async_copy(pool_ref.at[index_ref[j]], held.at[j], sems.at[j])

    @pl.when(step == 0)
    def _():
        def clear(layer, carry):
            filled[layer] = 0
            return carry

        lax.fori_loop(0, layers, clear, 0)
        dirty[0] = CAP

        def start(j, carry):
            fetch(j).start()
            layer = layer_ref[j]
            at = filled[layer]
            slots[layer * CAP + at] = j
            filled[layer] = at + 1
            return carry

        lax.fori_loop(0, live, start, 0)
        if peaks:
            acc, top = tops
            acc[...] = jnp.zeros_like(acc)
            top[...] = jnp.zeros_like(top)

        def wait(j, carry):
            fetch(j).wait()
            if peaks:
                layer = layer_ref[j]
                values = jnp.abs(held[j].astype(jnp.float32)).reshape(tokens // 8, 8, width)
                acc[layer] = jnp.maximum(acc[layer], jnp.max(values, axis=0))
            return carry

        lax.fori_loop(0, live, wait, 0)
        if peaks:
            whole = jnp.max(acc[...], axis=1)
            for h in range(SLICES):
                for n in range(pieces):
                    lanes = min(LANES, half - n * LANES)
                    at = h * half + n * LANES
                    top[h * pieces + n, :, :lanes] = whole[:, at : at + lanes]

    held_slots = filled[step]

    @pl.when(held_slots == 0)
    def _():
        for out in outs:
            out[...] = jnp.zeros_like(out)

    @pl.when(held_slots > 0)
    def _():
        def place(c, carry):
            values = held[slots[step * CAP + c], first_token:last_token, :].astype(jnp.float32)
            rows = pl.ds(pl.multiple_of(c * pitch, 8), here)
            for j in range(tiles):
                lanes = min(LANES, width - j * LANES)
                spread[j, rows, :lanes] = values[:, j * LANES : j * LANES + lanes]
            return carry

        lax.fori_loop(0, held_slots, place, 0)

        def blank(c, carry):
            for j in range(tiles):
                spread[j, pl.ds(pl.multiple_of(c * pitch, 8), here), :] = jnp.zeros((here, LANES), jnp.float32)
            return carry

        lax.fori_loop(held_slots, dirty[0], blank, 0)
        dirty[0] = held_slots

        lane = lax.broadcasted_iota(jnp.int32, (CAP, LANES), 1)
        if peaks:
            top = tops[1]
            row = lax.broadcasted_iota(jnp.int32, (CAP, LANES), 0)
            for h in range(SLICES):
                tile = jnp.zeros((CAP, LANES), jnp.float32)
                for n in range(pieces):
                    one = jnp.broadcast_to(top[h * pieces + n, pl.ds(step, 1), :], (CAP, LANES))
                    tile = jnp.where(row == n, one, tile)
                outs[0][h, :, counts[0] * group :] = tile.astype(jnp.bfloat16)

        for out, first, count in zip(outs, firsts, counts):

            def four_tokens(u, carry, out=out, first=first):
                at_row = QUAD * (u + first) - first_token
                rows = [
                    [spread[j, pl.ds(at_row + q, CAP, stride=pitch), :] for j in range(tiles)]
                    for q in range(QUAD)
                ]
                for h in range(SLICES):
                    turned = {}
                    for i in range(group // LANES):
                        whole, at = None, 0
                        while at < LANES:
                            flat = i * LANES + at
                            q = flat // half
                            source = flat - q * half + h * half
                            j = source // LANES
                            run = min(LANES - source % LANES, (q + 1) * half - flat, LANES - at)
                            if (q, j) not in turned:
                                shift = (at - source) % LANES
                                turned[q, j] = pltpu.roll(rows[q][j], shift, 1) if shift else rows[q][j]
                            piece = turned[q, j]
                            whole = piece if whole is None else jnp.where(lane >= at, piece, whole)
                            at += run
                        where = pl.ds(pl.multiple_of(u * group + i * LANES, LANES), LANES)
                        out[h, :, where] = whole.astype(jnp.bfloat16)
                return carry

            lax.fori_loop(0, count, four_tokens, 0, unroll=4)


def lay_out(block_pool, sel_index, sel_layer, counts, layers, firsts, groups, peaks):
    n_select = sel_index.shape[0]
    tokens, width = block_pool.shape[1:]
    half = width // SLICES
    tiles = pl.cdiv(width, LANES)
    here = QUAD * sum(groups)
    pitch = here + 8
    smem = pl.BlockSpec(memory_space=pltpu.SMEM)
    sizes = [QUAD * half * n for n in groups]
    scratch = [
        pltpu.VMEM((n_select, tokens, width), jnp.bfloat16),
        pltpu.VMEM((tiles, CAP * pitch, LANES), jnp.float32),
        pltpu.SMEM((layers * CAP,), jnp.int32),
        pltpu.SMEM((layers,), jnp.int32),
        pltpu.SMEM((1,), jnp.int32),
        pltpu.SemaphoreType.DMA((n_select,)),
    ]
    if peaks:
        sizes[0] += LANES
        scratch.append(pltpu.VMEM((layers, 8, width), jnp.float32))
        scratch.append(pltpu.VMEM((SLICES * pl.cdiv(half, LANES), layers, LANES), jnp.float32))
    return pl.pallas_call(
        functools.partial(lay_out_kernel, layers, firsts, groups, peaks),
        grid=(layers,),
        out_shape=[jax.ShapeDtypeStruct((layers * SLICES, CAP, n), jnp.bfloat16) for n in sizes],
        in_specs=[smem, smem, smem, pl.BlockSpec(memory_space=pl.ANY)],
        out_specs=[pl.BlockSpec((SLICES, CAP, n), lambda l: (l, 0, 0)) for n in sizes],
        scratch_shapes=scratch,
        cost_estimate=pl.CostEstimate(flops=100_000_000, bytes_accessed=20_000_000, transcendentals=0),
        name="lay_out",
    )(sel_index, sel_layer, counts, block_pool)


def code_kernel(coding, measuring, inverse_ref, raw_ref, *refs):
    sources, cap, lanes = raw_ref.shape
    tiles = lanes // LANES
    codes_ref = refs[-1 - measuring] if coding else None
    total_ref = refs[-1] if measuring else None
    inverse = [jnp.broadcast_to(inverse_ref[:, i * LANES : (i + 1) * LANES], (cap, LANES)) for i in range(tiles)]

    def source(s, totals):
        out = []
        for i in range(tiles):
            at = slice(i * LANES, (i + 1) * LANES)
            exact = raw_ref[s, :, at].astype(jnp.float32) * inverse[i]
            coded = jnp.clip(exact, -127.0, 127.0).astype(jnp.bfloat16)
            if coding:
                codes_ref[s, :, at] = coded
            if measuring:
                miss = exact - coded.astype(jnp.float32)
                out.append(totals[i] + miss * miss)
        return tuple(out)

    zeros = tuple(jnp.zeros((cap, LANES), jnp.float32) for _ in range(tiles)) if measuring else ()
    totals = lax.fori_loop(0, sources, source, zeros, unroll=2)
    if measuring:

        @pl.when(pl.program_id(0) == 0)
        def _():
            total_ref[...] = jnp.zeros_like(total_ref)

        for i in range(tiles):
            total_ref[:, i * LANES : (i + 1) * LANES] += totals[i]


def code(raw, inverse, codes, start, first, groups, all_groups, coding, measuring):
    sources, cap, _ = raw.shape
    lanes = inverse.shape[1]
    specs = [
        pl.BlockSpec((1, lanes), lambda u: (0, 0)),
        pl.BlockSpec((sources, cap, lanes), lambda u: (0, 0, start + u)),
    ]
    args = [inverse, raw]
    aliases = {}
    shapes, out_specs = [], []
    if coding:
        if codes is not None:
            specs.append(pl.BlockSpec(memory_space=pl.ANY))
            args.append(codes)
            aliases = {2: 0}
        shapes.append(jax.ShapeDtypeStruct((sources, cap, lanes * all_groups), jnp.bfloat16))
        out_specs.append(pl.BlockSpec((sources, cap, lanes), lambda u: (0, 0, first + u)))
    if measuring:
        shapes.append(jax.ShapeDtypeStruct((cap, lanes), jnp.float32))
        out_specs.append(pl.BlockSpec((cap, lanes), lambda u: (0, 0)))
    return pl.pallas_call(
        functools.partial(code_kernel, coding, measuring),
        grid=(groups,),
        out_shape=shapes,
        in_specs=specs,
        out_specs=out_specs,
        input_output_aliases=aliases,
        cost_estimate=pl.CostEstimate(flops=20_000_000 * groups, bytes_accessed=1_200_000 * groups, transcendentals=0),
        name="code" if coding else "measure",
    )(*args)


def over_rep(x, op):
    x = op(x, lax.ppermute(x, "rep", [(0, 1), (1, 0), (2, 3), (3, 2)]))
    return op(x, lax.ppermute(x, "rep", [(0, 3), (3, 0), (1, 2), (2, 1)]))


def body(block_pool, sel_index, sel_layer, counts):
    own_count = lax.axis_size("own")
    rep_count = lax.axis_size("rep")
    layers = own_count // SLICES
    tokens, width = block_pool.shape[1:]
    half = width // SLICES
    firsts = [sum(CHUNKS[:n]) for n in range(len(CHUNKS))]

    def exchange(x):
        return lax.all_to_all(x, "own", split_axis=0, concat_axis=0, tiled=True)

    sent = lay_out(block_pool, sel_index, sel_layer, counts, layers, firsts[:1], CHUNKS[:1], True)
    sent += lay_out(block_pool, sel_index, sel_layer, counts, layers, firsts[1:], CHUNKS[1:], False)
    early, late = [exchange(x) for x in sent]

    peak = jnp.max(early[:, :, QUAD * half * CHUNKS[0] :], axis=0).astype(jnp.float32)
    peak = over_rep(peak, jnp.maximum).reshape(1, CAP * LANES)[:, :half]
    steps = headroom * jnp.maximum(peak, 1.0) / 127.0
    inverse = jnp.tile(1.0 / steps, (1, QUAD))
    every = tokens // QUAD
    codes, error = code(early, inverse, None, 0, 0, CHUNKS[0], every, True, True)
    (more,) = code(late, inverse, None, 0, 0, CHUNKS[1], every, False, True)
    error = jnp.sum(error + more, axis=0).reshape(QUAD, half).sum(axis=0, keepdims=True)
    split = CHUNKS[1] // 2
    (codes,) = code(late, inverse, codes, 0, CHUNKS[0], split, every, True, False)
    (codes,) = code(late, inverse, codes, split, CHUNKS[0] + split, CHUNKS[1] - split, every, True, False)
    error = over_rep(error, jnp.add)
    denominator = float(own_count * rep_count * CAP * tokens)
    return codes[None, None], steps, error / denominator


def solution(mesh):
    return jax.shard_map(
        body,
        mesh=mesh,
        in_specs=(
            P(("own", "rep"), None, None),
            P(("own", "rep")),
            P(("own", "rep")),
            P(("own", "rep")),
        ),
        out_specs=(P("own", "rep", None, None, None), P("own", None), P("own", None)),
        check_vma=False,
    )
```

```python
import functools
import jax
import jax.numpy as jnp
from jax import lax
from jax.experimental import pallas as pl
from jax.experimental.pallas import tpu as pltpu
from jax.sharding import PartitionSpec as P

SLICES = 2
CAP = 8
LANES = 128
QUAD = 4
headroom = 0.5


def end_to_end(rows, width, start):
    lane = lax.broadcasted_iota(jnp.int32, rows[0][0].shape, 1)
    turned, out = {}, []
    for i in range(len(rows) * width // LANES):
        whole, at = None, 0
        while at < LANES:
            flat = i * LANES + at
            q = flat // width
            source = flat - q * width + start
            j = source // LANES
            run = min(LANES - source % LANES, (q + 1) * width - flat, LANES - at)
            if (q, j) not in turned:
                shift = (at - source) % LANES
                turned[q, j] = pltpu.roll(rows[q][j], shift, 1) if shift else rows[q][j]
            piece = turned[q, j]
            whole = piece if whole is None else jnp.where(lane >= at, piece, whole)
            at += run
        out.append(whole)
    return out


def peak_kernel(index_ref, layer_ref, count_ref, pool_ref, out_ref, held, acc, top, sems):
    live = count_ref[0]
    tokens, width = held.shape[1:]
    layers = acc.shape[0]
    half = width // SLICES
    pieces = top.shape[0] // SLICES

    def fetch(j):
        return pltpu.make_async_copy(pool_ref.at[index_ref[j]], held.at[j], sems.at[j])

    def start(j, carry):
        fetch(j).start()
        return carry

    lax.fori_loop(0, live, start, 0)
    acc[...] = jnp.zeros_like(acc)
    top[...] = jnp.zeros_like(top)

    def wait(j, carry):
        fetch(j).wait()
        layer = layer_ref[j]
        values = jnp.abs(held[j].astype(jnp.float32)).reshape(tokens // 8, 8, width)
        acc[layer] = jnp.maximum(acc[layer], jnp.max(values, axis=0))
        return carry

    lax.fori_loop(0, live, wait, 0)
    whole = jnp.max(acc[...], axis=1)
    for h in range(SLICES):
        for n in range(pieces):
            lanes = min(LANES, half - n * LANES)
            at = h * half + n * LANES
            top[h * pieces + n, :, :lanes] = whole[:, at : at + lanes]
    row = lax.broadcasted_iota(jnp.int32, (CAP, LANES), 0)

    def tiles(layer, carry):
        for h in range(SLICES):
            tile = jnp.zeros((CAP, LANES), jnp.float32)
            for n in range(pieces):
                one = jnp.broadcast_to(top[h * pieces + n, pl.ds(layer, 1), :], (CAP, LANES))
                tile = jnp.where(row == n, one, tile)
            out_ref[layer * SLICES + h] = tile.astype(jnp.bfloat16)
        return carry

    lax.fori_loop(0, layers, tiles, 0, unroll=4)


def local_peaks(block_pool, sel_index, sel_layer, counts, layers):
    n_select = sel_index.shape[0]
    tokens, width = block_pool.shape[1:]
    pieces = pl.cdiv(width // SLICES, LANES)
    smem = pl.BlockSpec(memory_space=pltpu.SMEM)
    return pl.pallas_call(
        peak_kernel,
        out_shape=jax.ShapeDtypeStruct((layers * SLICES, CAP, LANES), jnp.bfloat16),
        in_specs=[smem, smem, smem, pl.BlockSpec(memory_space=pl.ANY)],
        out_specs=pl.BlockSpec(memory_space=pltpu.VMEM),
        scratch_shapes=[
            pltpu.VMEM((n_select, tokens, width), jnp.bfloat16),
            pltpu.VMEM((layers, 8, width), jnp.float32),
            pltpu.VMEM((SLICES * pieces, layers, LANES), jnp.float32),
            pltpu.SemaphoreType.DMA((n_select,)),
        ],
        cost_estimate=pl.CostEstimate(flops=20_000_000, bytes_accessed=2_500_000, transcendentals=0),
        name="peaks",
    )(sel_index, sel_layer, counts, block_pool)


def lay_out_kernel(first, index_ref, layer_ref, count_ref, pool_ref, *refs):
    out, held, spread, slots, filled, dirty, sems = refs[-7:]
    step = pl.program_id(0)
    live = count_ref[0]
    layers = filled.shape[0]
    tokens, width = held.shape[1:]
    half = width // SLICES
    tiles = spread.shape[0]
    pitch = spread.shape[1] // CAP
    group = QUAD * half

    def fetch(j):
        return pltpu.make_async_copy(pool_ref.at[index_ref[j]], held.at[j], sems.at[j])

    @pl.when(step == 0)
    def _():
        for layer in range(layers):
            filled[layer] = 0
        dirty[0] = CAP

        def start(j, carry):
            layer = layer_ref[j] - first

            @pl.when((layer >= 0) & (layer < layers))
            def _():
                fetch(j).start()
                at = filled[layer]
                slots[layer * CAP + at] = j
                filled[layer] = at + 1

            return carry

        lax.fori_loop(0, live, start, 0)

    held_slots = filled[step]

    @pl.when(held_slots == 0)
    def _():
        out[...] = jnp.zeros_like(out)

    @pl.when(held_slots > 0)
    def _():
        def place(c, carry):
            j = slots[step * CAP + c]
            fetch(j).wait()
            values = held[j].astype(jnp.float32)
            rows = pl.ds(pl.multiple_of(c * pitch, 8), tokens)
            for i in range(tiles):
                lanes = min(LANES, width - i * LANES)
                spread[i, rows, :lanes] = values[:, i * LANES : i * LANES + lanes]
            return carry

        lax.fori_loop(0, held_slots, place, 0)

        def blank(c, carry):
            for i in range(tiles):
                spread[i, pl.ds(pl.multiple_of(c * pitch, 8), tokens), :] = jnp.zeros((tokens, LANES), jnp.float32)
            return carry

        lax.fori_loop(held_slots, dirty[0], blank, 0)
        dirty[0] = held_slots

        def four_tokens(u, carry):
            rows = [
                [spread[i, pl.ds(QUAD * u + q, CAP, stride=pitch), :] for i in range(tiles)] for q in range(QUAD)
            ]
            for h in range(SLICES):
                for i, tile in enumerate(end_to_end(rows, half, h * half)):
                    where = pl.ds(pl.multiple_of(u * group + i * LANES, LANES), LANES)
                    out[h, :, where] = tile.astype(jnp.bfloat16)
            return carry

        lax.fori_loop(0, tokens // QUAD, four_tokens, 0, unroll=4)


def lay_out(block_pool, sel_index, sel_layer, counts, out, first, layers, all_layers):
    n_select = sel_index.shape[0]
    tokens, width = block_pool.shape[1:]
    flat = tokens * (width // SLICES)
    pitch = tokens + 8
    smem = pl.BlockSpec(memory_space=pltpu.SMEM)
    specs = [smem, smem, smem, pl.BlockSpec(memory_space=pl.ANY)]
    args = [sel_index, sel_layer, counts, block_pool]
    if out is not None:
        specs.append(pl.BlockSpec(memory_space=pl.ANY))
        args.append(out)
    return pl.pallas_call(
        functools.partial(lay_out_kernel, first),
        grid=(layers,),
        out_shape=jax.ShapeDtypeStruct((all_layers * SLICES, CAP, flat + LANES), jnp.bfloat16),
        in_specs=specs,
        out_specs=pl.BlockSpec((SLICES, CAP, flat), lambda l: (first + l, 0, 0)),
        scratch_shapes=[
            pltpu.VMEM((n_select, tokens, width), jnp.bfloat16),
            pltpu.VMEM((pl.cdiv(width, LANES), CAP * pitch, LANES), jnp.float32),
            pltpu.SMEM((layers * CAP,), jnp.int32),
            pltpu.SMEM((layers,), jnp.int32),
            pltpu.SMEM((1,), jnp.int32),
            pltpu.SemaphoreType.DMA((n_select,)),
        ],
        input_output_aliases={} if out is None else {4: 0},
        cost_estimate=pl.CostEstimate(flops=50_000_000, bytes_accessed=6_000_000, transcendentals=0),
        name="lay_out",
    )(*args)


def append_kernel(tile_ref, _, out_ref):
    out_ref[...] = tile_ref[...]


def append(tile, out):
    groups, cap, lanes = tile.shape
    last = out.shape[2] // lanes - 1
    return pl.pallas_call(
        append_kernel,
        grid=(1,),
        out_shape=jax.ShapeDtypeStruct(out.shape, out.dtype),
        in_specs=[pl.BlockSpec((groups, cap, lanes), lambda i: (0, 0, 0)), pl.BlockSpec(memory_space=pl.ANY)],
        out_specs=pl.BlockSpec((groups, cap, lanes), lambda i: (0, 0, last)),
        input_output_aliases={1: 0},
        name="append",
    )(tile, out)


def measure_kernel(peak_ref, raw_ref, inverse_ref, steps_ref, error_ref, total):
    sources, cap, lanes = raw_ref.shape
    tiles = lanes // LANES
    half = lanes // QUAD
    step = pl.program_id(0)

    @pl.when(step == 0)
    def _():
        peak = jnp.max(peak_ref[...].astype(jnp.float32), axis=0)
        scale = headroom * jnp.maximum(peak, 1.0) / 127.0
        rows = [jnp.broadcast_to(scale[n : n + 1], (cap, LANES)) for n in range(pl.cdiv(half, LANES))]
        for n, row in enumerate(rows):
            size = min(LANES, half - n * LANES)
            steps_ref[:, n * LANES : n * LANES + size] = row[:1, :size]
        for i, tile in enumerate(end_to_end([rows] * QUAD, half, 0)):
            inverse_ref[:, i * LANES : (i + 1) * LANES] = 1.0 / tile
        total[...] = jnp.zeros_like(total)

    inverse = [inverse_ref[:, i * LANES : (i + 1) * LANES] for i in range(tiles)]

    def source(s, totals):
        out = []
        for i in range(tiles):
            exact = raw_ref[s, :, i * LANES : (i + 1) * LANES].astype(jnp.float32) * inverse[i]
            miss = exact - jnp.clip(exact, -127.0, 127.0).astype(jnp.bfloat16).astype(jnp.float32)
            out.append(totals[i] + miss * miss)
        return tuple(out)

    totals = lax.fori_loop(
        0, sources, source, tuple(total[:, i * LANES : (i + 1) * LANES] for i in range(tiles)), unroll=8
    )
    for i in range(tiles):
        total[:, i * LANES : (i + 1) * LANES] = totals[i]

    @pl.when(step == pl.num_programs(0) - 1)
    def _():
        whole = jnp.sum(total[...], axis=0, keepdims=True)
        error = whole[:, :half]
        for q in range(1, QUAD):
            error = error + whole[:, q * half : (q + 1) * half]
        error_ref[...] = error


def measure(raw, groups, half):
    sources, cap, _ = raw.shape
    lanes = QUAD * half
    return pl.pallas_call(
        measure_kernel,
        grid=(groups,),
        out_shape=[
            jax.ShapeDtypeStruct((cap, lanes), jnp.float32),
            jax.ShapeDtypeStruct((1, half), jnp.float32),
            jax.ShapeDtypeStruct((1, half), jnp.float32),
        ],
        in_specs=[
            pl.BlockSpec((sources, cap, LANES), lambda u: (0, 0, groups * lanes // LANES)),
            pl.BlockSpec((sources, cap, lanes), lambda u: (0, 0, u)),
        ],
        out_specs=[
            pl.BlockSpec((cap, lanes), lambda u: (0, 0)),
            pl.BlockSpec((1, half), lambda u: (0, 0)),
            pl.BlockSpec((1, half), lambda u: (0, 0)),
        ],
        scratch_shapes=[pltpu.VMEM((cap, lanes), jnp.float32)],
        cost_estimate=pl.CostEstimate(flops=20_000_000 * groups, bytes_accessed=600_000 * groups, transcendentals=0),
        name="measure",
    )(raw, raw)


def code_kernel(inverse_ref, raw_ref, *refs):
    codes_ref = refs[-1]
    sources, _, lanes = raw_ref.shape
    tiles = lanes // LANES
    inverse = [inverse_ref[:, i * LANES : (i + 1) * LANES] for i in range(tiles)]

    def source(s, carry):
        for i in range(tiles):
            at = slice(i * LANES, (i + 1) * LANES)
            exact = raw_ref[s, :, at].astype(jnp.float32) * inverse[i]
            codes_ref[s, :, at] = jnp.clip(exact, -127.0, 127.0).astype(jnp.bfloat16)
        return carry

    lax.fori_loop(0, sources, source, 0, unroll=8)


def code(raw, inverse, codes, first, groups, all_groups):
    sources, cap, _ = raw.shape
    lanes = inverse.shape[1]
    specs = [
        pl.BlockSpec((cap, lanes), lambda u: (0, 0)),
        pl.BlockSpec((sources, cap, lanes), lambda u: (0, 0, first + u)),
    ]
    args = [inverse, raw]
    if codes is not None:
        specs.append(pl.BlockSpec(memory_space=pl.ANY))
        args.append(codes)
    return pl.pallas_call(
        code_kernel,
        grid=(groups,),
        out_shape=jax.ShapeDtypeStruct((sources, cap, lanes * all_groups), jnp.bfloat16),
        in_specs=specs,
        out_specs=pl.BlockSpec((sources, cap, lanes), lambda u: (0, 0, first + u)),
        input_output_aliases={} if codes is None else {2: 0},
        cost_estimate=pl.CostEstimate(flops=20_000_000 * groups, bytes_accessed=1_200_000 * groups, transcendentals=0),
        name="code",
    )(*args)


def over_rep(x, op, beside):
    done = None
    for pairs, work in zip(([(0, 1), (1, 0), (2, 3), (3, 2)], [(0, 3), (3, 0), (1, 2), (2, 1)]), beside):
        other = lax.ppermute(x, "rep", pairs)
        done = work(done)
        x, done = lax.optimization_barrier((op(x, other), done))
    return x, done


def body(block_pool, sel_index, sel_layer, counts):
    own_count = lax.axis_size("own")
    rep_count = lax.axis_size("rep")
    layers = own_count // SLICES
    tokens, width = block_pool.shape[1:]
    half = width // SLICES
    selection = (block_pool, sel_index, sel_layer, counts)

    upper = layers // 2
    peak, sent = over_rep(
        local_peaks(*selection, layers),
        jnp.maximum,
        (
            lambda out: lay_out(*selection, out, 0, upper, layers),
            lambda out: lay_out(*selection, out, upper, layers - upper, layers),
        ),
    )
    sent = append(peak, sent)
    arrived = lax.all_to_all(sent, "own", split_axis=0, concat_axis=0, tiled=True)

    every = tokens // QUAD
    inverse, steps, error = measure(arrived, every, half)
    split = every // 2
    error, codes = over_rep(
        error,
        jnp.add,
        (
            lambda out: code(arrived, inverse, out, 0, split, every),
            lambda out: code(arrived, inverse, out, split, every - split, every),
        ),
    )
    denominator = float(own_count * rep_count * CAP * tokens)
    return codes[None, None], steps, error / denominator


def solution(mesh):
    return jax.shard_map(
        body,
        mesh=mesh,
        in_specs=(
            P(("own", "rep"), None, None),
            P(("own", "rep")),
            P(("own", "rep")),
            P(("own", "rep")),
        ),
        out_specs=(P("own", "rep", None, None, None), P("own", None), P("own", None)),
        check_vma=False,
    )
```

```python
import functools
import jax
import jax.numpy as jnp
from jax import lax
from jax.experimental import pallas as pl
from jax.experimental.pallas import tpu as pltpu
from jax.sharding import PartitionSpec as P

SLICES = 2
CAP = 8
LANES = 128
QUAD = 4
headroom = 0.5


def end_to_end(rows, width, start):
    lane = lax.broadcasted_iota(jnp.int32, rows[0][0].shape, 1)
    turned, out = {}, []
    for i in range(len(rows) * width // LANES):
        whole, at = None, 0
        while at < LANES:
            flat = i * LANES + at
            q = flat // width
            source = flat - q * width + start
            j = source // LANES
            run = min(LANES - source % LANES, (q + 1) * width - flat, LANES - at)
            if (q, j) not in turned:
                shift = (at - source) % LANES
                turned[q, j] = pltpu.roll(rows[q][j], shift, 1) if shift else rows[q][j]
            piece = turned[q, j]
            whole = piece if whole is None else jnp.where(lane >= at, piece, whole)
            at += run
        out.append(whole)
    return out


def peak_kernel(index_ref, layer_ref, count_ref, pool_ref, out_ref, held, acc, top, sems):
    live = count_ref[0]
    tokens, width = held.shape[1:]
    layers = acc.shape[0]
    half = width // SLICES
    pieces = top.shape[0] // SLICES

    def fetch(j):
        return pltpu.make_async_copy(pool_ref.at[index_ref[j]], held.at[j], sems.at[j])

    def start(j, carry):
        fetch(j).start()
        return carry

    lax.fori_loop(0, live, start, 0)
    acc[...] = jnp.zeros_like(acc)
    top[...] = jnp.zeros_like(top)

    def wait(j, carry):
        fetch(j).wait()
        layer = layer_ref[j]
        values = jnp.abs(held[j].astype(jnp.float32)).reshape(tokens // 8, 8, width)
        acc[layer] = jnp.maximum(acc[layer], jnp.max(values, axis=0))
        return carry

    lax.fori_loop(0, live, wait, 0)
    whole = jnp.max(acc[...], axis=1)
    for h in range(SLICES):
        for n in range(pieces):
            lanes = min(LANES, half - n * LANES)
            at = h * half + n * LANES
            top[h * pieces + n, :, :lanes] = whole[:, at : at + lanes]
    row = lax.broadcasted_iota(jnp.int32, (CAP, LANES), 0)

    def tiles(layer, carry):
        for h in range(SLICES):
            tile = jnp.zeros((CAP, LANES), jnp.float32)
            for n in range(pieces):
                one = jnp.broadcast_to(top[h * pieces + n, pl.ds(layer, 1), :], (CAP, LANES))
                tile = jnp.where(row == n, one, tile)
            out_ref[layer * SLICES + h] = tile.astype(jnp.bfloat16)
        return carry

    lax.fori_loop(0, layers, tiles, 0, unroll=4)


def local_peaks(block_pool, sel_index, sel_layer, counts, layers):
    n_select = sel_index.shape[0]
    tokens, width = block_pool.shape[1:]
    pieces = pl.cdiv(width // SLICES, LANES)
    smem = pl.BlockSpec(memory_space=pltpu.SMEM)
    return pl.pallas_call(
        peak_kernel,
        out_shape=jax.ShapeDtypeStruct((layers * SLICES, CAP, LANES), jnp.bfloat16),
        in_specs=[smem, smem, smem, pl.BlockSpec(memory_space=pl.ANY)],
        out_specs=pl.BlockSpec(memory_space=pltpu.VMEM),
        scratch_shapes=[
            pltpu.VMEM((n_select, tokens, width), jnp.bfloat16),
            pltpu.VMEM((layers, 8, width), jnp.float32),
            pltpu.VMEM((SLICES * pieces, layers, LANES), jnp.float32),
            pltpu.SemaphoreType.DMA((n_select,)),
        ],
        cost_estimate=pl.CostEstimate(flops=20_000_000, bytes_accessed=2_500_000, transcendentals=0),
        name="peaks",
    )(sel_index, sel_layer, counts, block_pool)


def lay_out_kernel(first, index_ref, layer_ref, count_ref, pool_ref, *refs):
    out_ref, built, held, spread, slots, filled, dirty, sems, out_sems = refs[-9:]
    live = count_ref[0]
    layers = filled.shape[0]
    tokens, width = held.shape[1:]
    half = width // SLICES
    tiles = spread.shape[0]
    pitch = spread.shape[1] // CAP
    group = QUAD * half

    def fetch(j):
        return pltpu.make_async_copy(pool_ref.at[index_ref[j]], held.at[j], sems.at[j])

    def send(layer):
        here = pl.ds(SLICES * layer, SLICES)
        there = pl.ds(SLICES * (first + layer), SLICES)
        return pltpu.make_async_copy(
            built.at[here], out_ref.at[there, :, pl.ds(0, tokens * half)], out_sems.at[layer]
        )

    for layer in range(layers):
        filled[layer] = 0
    dirty[0] = CAP

    def start(j, carry):
        layer = layer_ref[j] - first

        @pl.when((layer >= 0) & (layer < layers))
        def _():
            fetch(j).start()
            at = filled[layer]
            slots[layer * CAP + at] = j
            filled[layer] = at + 1

        return carry

    lax.fori_loop(0, live, start, 0)

    def build(layer, carry):
        held_slots = filled[layer]

        @pl.when(held_slots == 0)
        def _():
            built[pl.ds(SLICES * layer, SLICES)] = jnp.zeros((SLICES, *built.shape[1:]), built.dtype)

        @pl.when(held_slots > 0)
        def _():
            def place(c, carry):
                j = slots[layer * CAP + c]
                fetch(j).wait()
                values = held[j].astype(jnp.float32)
                rows = pl.ds(pl.multiple_of(c * pitch, 8), tokens)
                for i in range(tiles):
                    lanes = min(LANES, width - i * LANES)
                    spread[i, rows, :lanes] = values[:, i * LANES : i * LANES + lanes]
                return carry

            lax.fori_loop(0, held_slots, place, 0)

            def blank(c, carry):
                for i in range(tiles):
                    spread[i, pl.ds(pl.multiple_of(c * pitch, 8), tokens), :] = jnp.zeros((tokens, LANES), jnp.float32)
                return carry

            lax.fori_loop(held_slots, dirty[0], blank, 0)
            dirty[0] = held_slots

            def four_tokens(u, carry):
                rows = [
                    [spread[i, pl.ds(QUAD * u + q, CAP, stride=pitch), :] for i in range(tiles)] for q in range(QUAD)
                ]
                for h in range(SLICES):
                    for i, tile in enumerate(end_to_end(rows, half, h * half)):
                        where = pl.ds(pl.multiple_of(u * group + i * LANES, LANES), LANES)
                        built[SLICES * layer + h, :, where] = tile.astype(jnp.bfloat16)
                return carry

            lax.fori_loop(0, tokens // QUAD, four_tokens, 0, unroll=4)

        send(layer).start()
        return carry

    lax.fori_loop(0, layers, build, 0)

    def finish(layer, carry):
        send(layer).wait()
        return carry

    lax.fori_loop(0, layers, finish, 0)


def lay_out(block_pool, sel_index, sel_layer, counts, out, first, layers, all_layers):
    n_select = sel_index.shape[0]
    tokens, width = block_pool.shape[1:]
    flat = tokens * (width // SLICES)
    pitch = tokens + 8
    smem = pl.BlockSpec(memory_space=pltpu.SMEM)
    hbm = pl.BlockSpec(memory_space=pl.ANY)
    specs = [smem, smem, smem, hbm]
    args = [sel_index, sel_layer, counts, block_pool]
    if out is not None:
        specs.append(hbm)
        args.append(out)
    return pl.pallas_call(
        functools.partial(lay_out_kernel, first),
        out_shape=jax.ShapeDtypeStruct((all_layers * SLICES, CAP, flat + LANES), jnp.bfloat16),
        in_specs=specs,
        out_specs=hbm,
        scratch_shapes=[
            pltpu.VMEM((layers * SLICES, CAP, flat), jnp.bfloat16),
            pltpu.VMEM((n_select, tokens, width), jnp.bfloat16),
            pltpu.VMEM((pl.cdiv(width, LANES), CAP * pitch, LANES), jnp.float32),
            pltpu.SMEM((layers * CAP,), jnp.int32),
            pltpu.SMEM((layers,), jnp.int32),
            pltpu.SMEM((1,), jnp.int32),
            pltpu.SemaphoreType.DMA((n_select,)),
            pltpu.SemaphoreType.DMA((layers,)),
        ],
        input_output_aliases={} if out is None else {4: 0},
        cost_estimate=pl.CostEstimate(flops=50_000_000, bytes_accessed=6_000_000, transcendentals=0),
        name="lay_out",
    )(*args)


def append_kernel(mine_ref, other_ref, _, out_ref, tile, sem):
    tile[...] = jnp.maximum(mine_ref[...], other_ref[...])
    lanes = tile.shape[2]
    copy = pltpu.make_async_copy(tile, out_ref.at[:, :, pl.ds(out_ref.shape[2] - lanes, lanes)], sem)
    copy.start()
    copy.wait()


def append(mine, other, out):
    vmem = pl.BlockSpec(memory_space=pltpu.VMEM)
    hbm = pl.BlockSpec(memory_space=pl.ANY)
    return pl.pallas_call(
        append_kernel,
        out_shape=jax.ShapeDtypeStruct(out.shape, out.dtype),
        in_specs=[vmem, vmem, hbm],
        out_specs=hbm,
        scratch_shapes=[pltpu.VMEM(mine.shape, mine.dtype), pltpu.SemaphoreType.DMA],
        input_output_aliases={2: 0},
        name="append",
    )(mine, other, out)


BATCH = 2


def encode_kernel(raw_ref, codes_ref, steps_ref, error_ref, peaks, raw, codes, inverse, peak_sem, in_sems, out_sems):
    sources, cap, _ = raw.shape
    lanes = inverse.shape[1]
    half = lanes // QUAD
    tiles = lanes // LANES
    flat = codes.shape[2]
    batches = sources // BATCH

    def take(b):
        here = pl.ds(b * BATCH, BATCH)
        return pltpu.make_async_copy(raw_ref.at[here, :, pl.ds(0, flat)], raw.at[here], in_sems.at[b])

    def give(b):
        here = pl.ds(b * BATCH, BATCH)
        return pltpu.make_async_copy(codes.at[here], codes_ref.at[here], out_sems.at[b])

    take_peaks = pltpu.make_async_copy(raw_ref.at[:, :, pl.ds(flat, LANES)], peaks, peak_sem)
    take_peaks.start()
    for b in range(batches):
        take(b).start()
    take_peaks.wait()
    peak = jnp.max(peaks[...].astype(jnp.float32), axis=0)
    scale = headroom * jnp.maximum(peak, 1.0) / 127.0
    rows = [jnp.broadcast_to(scale[n : n + 1], (cap, LANES)) for n in range(pl.cdiv(half, LANES))]
    for n, row in enumerate(rows):
        size = min(LANES, half - n * LANES)
        steps_ref[:, n * LANES : n * LANES + size] = row[:1, :size]
    for i, tile in enumerate(end_to_end([rows] * QUAD, half, 0)):
        inverse[:, i * LANES : (i + 1) * LANES] = 1.0 / tile
    by_lane = [inverse[:, i * LANES : (i + 1) * LANES] for i in range(tiles)]

    def batch(b, totals):
        take(b).wait()

        def group(u, totals):
            totals = list(totals)
            for i in range(tiles):
                at = pl.ds(pl.multiple_of(u * lanes + i * LANES, LANES), LANES)
                for s in range(BATCH):
                    exact = raw[b * BATCH + s, :, at].astype(jnp.float32) * by_lane[i]
                    coded = jnp.clip(exact, -127.0, 127.0).astype(jnp.bfloat16)
                    codes[b * BATCH + s, :, at] = coded
                    miss = exact - coded.astype(jnp.float32)
                    totals[i] = totals[i] + miss * miss
            return tuple(totals)

        totals = lax.fori_loop(0, flat // lanes, group, totals, unroll=4)
        give(b).start()
        return totals

    totals = lax.fori_loop(
        0, batches, batch, tuple(jnp.zeros((cap, LANES), jnp.float32) for _ in range(tiles))
    )
    whole = jnp.concatenate([jnp.sum(t, axis=0, keepdims=True) for t in totals], axis=1)
    error = whole[:, :half]
    for q in range(1, QUAD):
        error = error + whole[:, q * half : (q + 1) * half]
    error_ref[...] = error
    for b in range(batches):
        give(b).wait()


def encode(raw, half):
    sources, cap, size = raw.shape
    flat = size - LANES
    vmem = pl.BlockSpec(memory_space=pltpu.VMEM)
    hbm = pl.BlockSpec(memory_space=pl.ANY)
    return pl.pallas_call(
        encode_kernel,
        out_shape=[
            jax.ShapeDtypeStruct((sources, cap, flat), jnp.bfloat16),
            jax.ShapeDtypeStruct((1, half), jnp.float32),
            jax.ShapeDtypeStruct((1, half), jnp.float32),
        ],
        in_specs=[hbm],
        out_specs=[hbm, vmem, vmem],
        scratch_shapes=[
            pltpu.VMEM((sources, cap, LANES), jnp.bfloat16),
            pltpu.VMEM((sources, cap, flat), jnp.bfloat16),
            pltpu.VMEM((sources, cap, flat), jnp.bfloat16),
            pltpu.VMEM((cap, QUAD * half), jnp.float32),
            pltpu.SemaphoreType.DMA,
            pltpu.SemaphoreType.DMA((sources // BATCH,)),
            pltpu.SemaphoreType.DMA((sources // BATCH,)),
        ],
        cost_estimate=pl.CostEstimate(flops=80_000_000, bytes_accessed=19_000_000, transcendentals=0),
        name="encode",
    )(raw)


NEIGHBOURS = ([(0, 1), (1, 0), (2, 3), (3, 2)], [(0, 3), (3, 0), (1, 2), (2, 1)])


def body(block_pool, sel_index, sel_layer, counts):
    own_count = lax.axis_size("own")
    rep_count = lax.axis_size("rep")
    layers = own_count // SLICES
    tokens, width = block_pool.shape[1:]
    half = width // SLICES
    selection = (block_pool, sel_index, sel_layer, counts)

    upper = layers // 2
    peak = local_peaks(*selection, layers)
    other = lax.ppermute(peak, "rep", NEIGHBOURS[0])
    sent = lay_out(*selection, None, 0, upper, layers)
    peak, sent = lax.optimization_barrier((jnp.maximum(peak, other), sent))
    other = lax.ppermute(peak, "rep", NEIGHBOURS[1])
    sent = lay_out(*selection, sent, upper, layers - upper, layers)
    sent = append(peak, other, sent)
    arrived = lax.all_to_all(sent, "own", split_axis=0, concat_axis=0, tiled=True)

    codes, steps, error = encode(arrived, half)
    for pairs in NEIGHBOURS:
        error = error + lax.ppermute(error, "rep", pairs)
    denominator = float(own_count * rep_count * CAP * tokens)
    return codes[None, None], steps, error / denominator


def solution(mesh):
    return jax.shard_map(
        body,
        mesh=mesh,
        in_specs=(
            P(("own", "rep"), None, None),
            P(("own", "rep")),
            P(("own", "rep")),
            P(("own", "rep")),
        ),
        out_specs=(P("own", "rep", None, None, None), P("own", None), P("own", None)),
        check_vma=False,
    )
```

```python
import functools
import jax
import jax.numpy as jnp
from jax import lax
from jax.experimental import pallas as pl
from jax.experimental.pallas import tpu as pltpu
from jax.sharding import PartitionSpec as P

SLICES = 2
CAP = 8
LANES = 128
QUAD = 4
headroom = 0.5


def end_to_end(rows, width, start):
    lane = lax.broadcasted_iota(jnp.int32, rows[0][0].shape, 1)
    turned, out = {}, []
    for i in range(len(rows) * width // LANES):
        whole, at = None, 0
        while at < LANES:
            flat = i * LANES + at
            q = flat // width
            source = flat - q * width + start
            j = source // LANES
            run = min(LANES - source % LANES, (q + 1) * width - flat, LANES - at)
            if (q, j) not in turned:
                shift = (at - source) % LANES
                turned[q, j] = pltpu.roll(rows[q][j], shift, 1) if shift else rows[q][j]
            piece = turned[q, j]
            whole = piece if whole is None else jnp.where(lane >= at, piece, whole)
            at += run
        out.append(whole)
    return out


def peak_kernel(index_ref, layer_ref, count_ref, pool_ref, out_ref, held, acc, top, sems):
    live = count_ref[0]
    tokens, width = held.shape[1:]
    layers = acc.shape[0]
    half = width // SLICES
    pieces = top.shape[0] // SLICES

    def fetch(j):
        return pltpu.make_async_copy(pool_ref.at[index_ref[j]], held.at[j], sems.at[j])

    def start(j, carry):
        fetch(j).start()
        return carry

    lax.fori_loop(0, live, start, 0)
    acc[...] = jnp.zeros_like(acc)
    top[...] = jnp.zeros_like(top)

    def wait(j, carry):
        fetch(j).wait()
        layer = layer_ref[j]
        values = jnp.abs(held[j].astype(jnp.float32)).reshape(tokens // 8, 8, width)
        acc[layer] = jnp.maximum(acc[layer], jnp.max(values, axis=0))
        return carry

    lax.fori_loop(0, live, wait, 0)
    whole = jnp.max(acc[...], axis=1)
    for h in range(SLICES):
        for n in range(pieces):
            lanes = min(LANES, half - n * LANES)
            at = h * half + n * LANES
            top[h * pieces + n, :, :lanes] = whole[:, at : at + lanes]
    row = lax.broadcasted_iota(jnp.int32, (CAP, LANES), 0)

    def tiles(layer, carry):
        for h in range(SLICES):
            tile = jnp.zeros((CAP, LANES), jnp.float32)
            for n in range(pieces):
                one = jnp.broadcast_to(top[h * pieces + n, pl.ds(layer, 1), :], (CAP, LANES))
                tile = jnp.where(row == n, one, tile)
            out_ref[layer * SLICES + h] = tile.astype(jnp.bfloat16)
        return carry

    lax.fori_loop(0, layers, tiles, 0, unroll=4)


def local_peaks(block_pool, sel_index, sel_layer, counts, layers):
    n_select = sel_index.shape[0]
    tokens, width = block_pool.shape[1:]
    pieces = pl.cdiv(width // SLICES, LANES)
    smem = pl.BlockSpec(memory_space=pltpu.SMEM)
    return pl.pallas_call(
        peak_kernel,
        out_shape=jax.ShapeDtypeStruct((layers * SLICES, CAP, LANES), jnp.bfloat16),
        in_specs=[smem, smem, smem, pl.BlockSpec(memory_space=pl.ANY)],
        out_specs=pl.BlockSpec(memory_space=pltpu.VMEM),
        scratch_shapes=[
            pltpu.VMEM((n_select, tokens, width), jnp.bfloat16),
            pltpu.VMEM((layers, 8, width), jnp.float32),
            pltpu.VMEM((SLICES * pieces, layers, LANES), jnp.float32),
            pltpu.SemaphoreType.DMA((n_select,)),
        ],
        cost_estimate=pl.CostEstimate(flops=20_000_000, bytes_accessed=2_500_000, transcendentals=0),
        name="peaks",
    )(sel_index, sel_layer, counts, block_pool)


def lay_out_kernel(
    index_ref, layer_ref, count_ref, pool_ref, out_ref, built, held, spread, slots, filled, dirty, sems, out_sems
):
    live = count_ref[0]
    layers = filled.shape[0]
    tokens, width = held.shape[1:]
    half = width // SLICES
    tiles = spread.shape[0]
    pitch = spread.shape[1] // CAP
    group = QUAD * half

    def fetch(j):
        return pltpu.make_async_copy(pool_ref.at[index_ref[j]], held.at[j], sems.at[j])

    def send(layer):
        here = pl.ds(SLICES * layer, SLICES)
        return pltpu.make_async_copy(
            built.at[here], out_ref.at[here, :, pl.ds(0, tokens * half)], out_sems.at[layer]
        )

    for layer in range(layers):
        filled[layer] = 0
    dirty[0] = CAP

    def start(j, carry):
        fetch(j).start()
        layer = layer_ref[j]
        at = filled[layer]
        slots[layer * CAP + at] = j
        filled[layer] = at + 1
        return carry

    lax.fori_loop(0, live, start, 0)

    def build(layer, carry):
        held_slots = filled[layer]

        @pl.when(held_slots == 0)
        def _():
            built[pl.ds(SLICES * layer, SLICES)] = jnp.zeros((SLICES, *built.shape[1:]), built.dtype)

        @pl.when(held_slots > 0)
        def _():
            def place(c, carry):
                j = slots[layer * CAP + c]
                fetch(j).wait()
                values = held[j].astype(jnp.float32)
                rows = pl.ds(pl.multiple_of(c * pitch, 8), tokens)
                for i in range(tiles):
                    lanes = min(LANES, width - i * LANES)
                    spread[i, rows, :lanes] = values[:, i * LANES : i * LANES + lanes]
                return carry

            lax.fori_loop(0, held_slots, place, 0)

            def blank(c, carry):
                for i in range(tiles):
                    spread[i, pl.ds(pl.multiple_of(c * pitch, 8), tokens), :] = jnp.zeros((tokens, LANES), jnp.float32)
                return carry

            lax.fori_loop(held_slots, dirty[0], blank, 0)
            dirty[0] = held_slots

            def four_tokens(u, carry):
                rows = [
                    [spread[i, pl.ds(QUAD * u + q, CAP, stride=pitch), :] for i in range(tiles)] for q in range(QUAD)
                ]
                for h in range(SLICES):
                    for i, tile in enumerate(end_to_end(rows, half, h * half)):
                        where = pl.ds(pl.multiple_of(u * group + i * LANES, LANES), LANES)
                        built[SLICES * layer + h, :, where] = tile.astype(jnp.bfloat16)
                return carry

            lax.fori_loop(0, tokens // QUAD, four_tokens, 0, unroll=tokens // QUAD)

        send(layer).start()
        return carry

    lax.fori_loop(0, layers, build, 0)

    def finish(layer, carry):
        send(layer).wait()
        return carry

    lax.fori_loop(0, layers, finish, 0)


def lay_out(block_pool, sel_index, sel_layer, counts, layers):
    n_select = sel_index.shape[0]
    tokens, width = block_pool.shape[1:]
    flat = tokens * (width // SLICES)
    pitch = tokens + 8
    smem = pl.BlockSpec(memory_space=pltpu.SMEM)
    hbm = pl.BlockSpec(memory_space=pl.ANY)
    return pl.pallas_call(
        lay_out_kernel,
        out_shape=jax.ShapeDtypeStruct((layers * SLICES, CAP, flat + LANES), jnp.bfloat16),
        in_specs=[smem, smem, smem, hbm],
        out_specs=hbm,
        scratch_shapes=[
            pltpu.VMEM((layers * SLICES, CAP, flat), jnp.bfloat16),
            pltpu.VMEM((n_select, tokens, width), jnp.bfloat16),
            pltpu.VMEM((pl.cdiv(width, LANES), CAP * pitch, LANES), jnp.float32),
            pltpu.SMEM((layers * CAP,), jnp.int32),
            pltpu.SMEM((layers,), jnp.int32),
            pltpu.SMEM((1,), jnp.int32),
            pltpu.SemaphoreType.DMA((n_select,)),
            pltpu.SemaphoreType.DMA((layers,)),
        ],
        cost_estimate=pl.CostEstimate(flops=200_000_000, bytes_accessed=12_000_000, transcendentals=0),
        name="lay_out",
    )(sel_index, sel_layer, counts, block_pool)


BATCH = 4
AHEAD = 3


def encode_kernel(raw_ref, codes_ref, steps_ref, error_ref, peaks, raw, codes, inverse, peak_sem, in_sems, out_sems):
    sources, cap, _ = raw.shape
    lanes = inverse.shape[1]
    half = lanes // QUAD
    tiles = lanes // LANES
    flat = codes.shape[2]
    batches = sources // BATCH

    def take(b):
        here = pl.ds(b * BATCH, BATCH)
        return pltpu.make_async_copy(raw_ref.at[here, :, pl.ds(0, flat)], raw.at[here], in_sems.at[b])

    def give(b):
        here = pl.ds(b * BATCH, BATCH)
        return pltpu.make_async_copy(codes.at[here], codes_ref.at[here], out_sems.at[b])

    take_peaks = pltpu.make_async_copy(raw_ref.at[:, :, pl.ds(flat, LANES)], peaks, peak_sem)
    take_peaks.start()
    for b in range(AHEAD):
        take(b).start()
    take_peaks.wait()
    peak = jnp.max(peaks[...].astype(jnp.float32), axis=0)
    scale = headroom * jnp.maximum(peak, 1.0) / 127.0
    rows = [jnp.broadcast_to(scale[n : n + 1], (cap, LANES)) for n in range(pl.cdiv(half, LANES))]
    for n, row in enumerate(rows):
        size = min(LANES, half - n * LANES)
        steps_ref[:, n * LANES : n * LANES + size] = row[:1, :size]
    for i, tile in enumerate(end_to_end([rows] * QUAD, half, 0)):
        inverse[:, i * LANES : (i + 1) * LANES] = 1.0 / tile
    by_lane = [inverse[:, i * LANES : (i + 1) * LANES] for i in range(tiles)]

    def batch(b, totals):
        take(b).wait()

        @pl.when(b + AHEAD < batches)
        def _():
            take(b + AHEAD).start()


        def group(u, totals):
            totals = list(totals)
            for i in range(tiles):
                at = pl.ds(pl.multiple_of(u * lanes + i * LANES, LANES), LANES)
                for s in range(BATCH):
                    exact = raw[b * BATCH + s, :, at].astype(jnp.float32) * by_lane[i]
                    coded = jnp.clip(exact, -127.0, 127.0).astype(jnp.bfloat16)
                    codes[b * BATCH + s, :, at] = coded
                    miss = exact - coded.astype(jnp.float32)
                    totals[i] = totals[i] + miss * miss
            return tuple(totals)

        totals = lax.fori_loop(0, flat // lanes, group, totals, unroll=4)
        give(b).start()
        return totals

    totals = lax.fori_loop(
        0, batches, batch, tuple(jnp.zeros((cap, LANES), jnp.float32) for _ in range(tiles))
    )
    whole = jnp.concatenate([jnp.sum(t, axis=0, keepdims=True) for t in totals], axis=1)
    error = whole[:, :half]
    for q in range(1, QUAD):
        error = error + whole[:, q * half : (q + 1) * half]
    error_ref[...] = error
    for b in range(batches):
        give(b).wait()


def encode(raw, half):
    sources, cap, size = raw.shape
    flat = size - LANES
    vmem = pl.BlockSpec(memory_space=pltpu.VMEM)
    hbm = pl.BlockSpec(memory_space=pl.ANY)
    return pl.pallas_call(
        encode_kernel,
        out_shape=[
            jax.ShapeDtypeStruct((sources, cap, flat), jnp.bfloat16),
            jax.ShapeDtypeStruct((1, half), jnp.float32),
            jax.ShapeDtypeStruct((1, half), jnp.float32),
        ],
        in_specs=[hbm],
        out_specs=[hbm, vmem, vmem],
        scratch_shapes=[
            pltpu.VMEM((sources, cap, LANES), jnp.bfloat16),
            pltpu.VMEM((sources, cap, flat), jnp.bfloat16),
            pltpu.VMEM((sources, cap, flat), jnp.bfloat16),
            pltpu.VMEM((cap, QUAD * half), jnp.float32),
            pltpu.SemaphoreType.DMA,
            pltpu.SemaphoreType.DMA((sources // BATCH,)),
            pltpu.SemaphoreType.DMA((sources // BATCH,)),
        ],
        cost_estimate=pl.CostEstimate(flops=80_000_000, bytes_accessed=19_000_000, transcendentals=0),
        name="encode",
    )(raw)


NEIGHBOURS = ([(0, 1), (1, 0), (2, 3), (3, 2)], [(0, 3), (3, 0), (1, 2), (2, 1)])


def body(block_pool, sel_index, sel_layer, counts):
    own_count = lax.axis_size("own")
    rep_count = lax.axis_size("rep")
    layers = own_count // SLICES
    tokens, width = block_pool.shape[1:]
    half = width // SLICES
    selection = (block_pool, sel_index, sel_layer, counts)

    peak = local_peaks(*selection, layers)
    others = [lax.ppermute(peak, "rep", [(r, (r + k) % rep_count) for r in range(rep_count)]) for k in range(1, rep_count)]
    sent = lay_out(*selection, layers)
    peak = functools.reduce(jnp.maximum, others, peak)
    sent = lax.dynamic_update_slice(sent, peak, (0, 0, tokens * half))
    arrived = lax.all_to_all(sent, "own", split_axis=0, concat_axis=0, tiled=True)

    codes, steps, error = encode(arrived, half)
    for pairs in NEIGHBOURS:
        error = error + lax.ppermute(error, "rep", pairs)
    denominator = float(own_count * rep_count * CAP * tokens)
    return codes[None, None], steps, error / denominator


def solution(mesh):
    return jax.shard_map(
        body,
        mesh=mesh,
        in_specs=(
            P(("own", "rep"), None, None),
            P(("own", "rep")),
            P(("own", "rep")),
            P(("own", "rep")),
        ),
        out_specs=(P("own", "rep", None, None, None), P("own", None), P("own", None)),
        check_vma=False,
    )
```

```python
import functools
import jax
import jax.numpy as jnp
from jax import lax
from jax.experimental import pallas as pl
from jax.experimental.pallas import tpu as pltpu
from jax.sharding import PartitionSpec as P

SLICES = 2
CAP = 8
LANES = 128
QUAD = 4
headroom = 0.5
VMEM_LIMIT = 30 * 2**20


def end_to_end(rows, width, start):
    lane = lax.broadcasted_iota(jnp.int32, rows[0][0].shape, 1)
    turned, out = {}, []
    for i in range(len(rows) * width // LANES):
        whole, at = None, 0
        while at < LANES:
            flat = i * LANES + at
            q = flat // width
            source = flat - q * width + start
            j = source // LANES
            run = min(LANES - source % LANES, (q + 1) * width - flat, LANES - at)
            if (q, j) not in turned:
                shift = (at - source) % LANES
                turned[q, j] = pltpu.roll(rows[q][j], shift, 1) if shift else rows[q][j]
            piece = turned[q, j]
            whole = piece if whole is None else jnp.where(lane >= at, piece, whole)
            at += run
        out.append(whole)
    return out


def peak_kernel(index_ref, layer_ref, count_ref, pool_ref, out_ref, held, slots, filled, acc, top, sems):
    live = count_ref[0]
    tokens, width = held.shape[1:]
    layers = acc.shape[0]
    half = width // SLICES
    pieces = top.shape[0] // SLICES

    def fetch(j):
        return pltpu.make_async_copy(pool_ref.at[index_ref[j]], held.at[j], sems.at[j])

    for layer in range(layers):
        filled[layer] = 0

    def start(j, carry):
        fetch(j).start()
        layer = layer_ref[j]
        at = filled[layer]
        slots[layer * CAP + at] = j
        filled[layer] = at + 1
        return carry

    lax.fori_loop(0, live, start, 0)
    acc[...] = jnp.zeros_like(acc)
    top[...] = jnp.zeros_like(top)

    def wait(j, carry):
        fetch(j).wait()
        layer = layer_ref[j]
        values = jnp.abs(held[j].astype(jnp.float32)).reshape(tokens // 8, 8, width)
        acc[layer] = jnp.maximum(acc[layer], jnp.max(values, axis=0))
        return carry

    lax.fori_loop(0, live, wait, 0)
    whole = jnp.max(acc[...], axis=1)
    for h in range(SLICES):
        for n in range(pieces):
            lanes = min(LANES, half - n * LANES)
            at = h * half + n * LANES
            top[h * pieces + n, :, :lanes] = whole[:, at : at + lanes]
    row = lax.broadcasted_iota(jnp.int32, (CAP, LANES), 0)

    def tiles(layer, carry):
        for h in range(SLICES):
            tile = jnp.zeros((CAP, LANES), jnp.float32)
            for n in range(pieces):
                one = jnp.broadcast_to(top[h * pieces + n, pl.ds(layer, 1), :], (CAP, LANES))
                tile = jnp.where(row == n, one, tile)
            out_ref[layer * SLICES + h] = tile.astype(jnp.bfloat16)
        return carry

    lax.fori_loop(0, layers, tiles, 0, unroll=4)


def local_peaks(block_pool, sel_index, sel_layer, counts, layers):
    n_select = sel_index.shape[0]
    tokens, width = block_pool.shape[1:]
    pieces = pl.cdiv(width // SLICES, LANES)
    smem = pl.BlockSpec(memory_space=pltpu.SMEM)
    vmem = pl.BlockSpec(memory_space=pltpu.VMEM)
    return pl.pallas_call(
        peak_kernel,
        out_shape=[
            pltpu.VMEM((layers * SLICES, CAP, LANES), jnp.bfloat16),
            pltpu.VMEM((n_select, tokens, width), jnp.bfloat16),
            pltpu.SMEM((layers * CAP,), jnp.int32),
            pltpu.SMEM((layers,), jnp.int32),
        ],
        in_specs=[smem, smem, smem, pl.BlockSpec(memory_space=pltpu.HBM)],
        out_specs=[vmem, vmem, smem, smem],
        scratch_shapes=[
            pltpu.VMEM((layers, 8, width), jnp.float32),
            pltpu.VMEM((SLICES * pieces, layers, LANES), jnp.float32),
            pltpu.SemaphoreType.DMA((n_select,)),
        ],
        compiler_params=pltpu.CompilerParams(vmem_limit_bytes=2 * VMEM_LIMIT),
        cost_estimate=pl.CostEstimate(flops=20_000_000, bytes_accessed=2_500_000, transcendentals=0),
        name="peaks",
    )(sel_index, sel_layer, counts, block_pool)


def lay_out_kernel(slots, filled, held, built, spread, dirty):
    layers = filled.shape[0]
    tokens, width = held.shape[1:]
    half = width // SLICES
    tiles = spread.shape[0]
    pitch = spread.shape[1] // CAP
    group = QUAD * half
    dirty[0] = CAP

    def build(layer, carry):
        held_slots = filled[layer]

        @pl.when(held_slots == 0)
        def _():
            built[pl.ds(SLICES * layer, SLICES), :, : tokens * half] = jnp.zeros(
                (SLICES, CAP, tokens * half), built.dtype
            )

        @pl.when(held_slots > 0)
        def _():
            def place(c, carry):
                values = held[slots[layer * CAP + c]].astype(jnp.float32)
                rows = pl.ds(pl.multiple_of(c * pitch, 8), tokens)
                for i in range(tiles):
                    lanes = min(LANES, width - i * LANES)
                    spread[i, rows, :lanes] = values[:, i * LANES : i * LANES + lanes]
                return carry

            lax.fori_loop(0, held_slots, place, 0)

            def blank(c, carry):
                for i in range(tiles):
                    spread[i, pl.ds(pl.multiple_of(c * pitch, 8), tokens), :] = jnp.zeros((tokens, LANES), jnp.float32)
                return carry

            lax.fori_loop(held_slots, dirty[0], blank, 0)
            dirty[0] = held_slots

            def four_tokens(u, carry):
                rows = [
                    [spread[i, pl.ds(QUAD * u + q, CAP, stride=pitch), :] for i in range(tiles)] for q in range(QUAD)
                ]
                for h in range(SLICES):
                    for i, tile in enumerate(end_to_end(rows, half, h * half)):
                        where = pl.ds(pl.multiple_of(u * group + i * LANES, LANES), LANES)
                        built[SLICES * layer + h, :, where] = tile.astype(jnp.bfloat16)
                return carry

            lax.fori_loop(0, tokens // QUAD, four_tokens, 0, unroll=tokens // QUAD)

        return carry

    lax.fori_loop(0, layers, build, 0)


def lay_out(held, slots, filled):
    layers = filled.shape[0]
    _, tokens, width = held.shape
    flat = tokens * (width // SLICES)
    pitch = tokens + 8
    smem = pl.BlockSpec(memory_space=pltpu.SMEM)
    vmem = pl.BlockSpec(memory_space=pltpu.VMEM)
    return pl.pallas_call(
        lay_out_kernel,
        out_shape=pltpu.VMEM((layers * SLICES, CAP, flat + LANES), jnp.bfloat16),
        in_specs=[smem, smem, vmem],
        out_specs=vmem,
        scratch_shapes=[
            pltpu.VMEM((pl.cdiv(width, LANES), CAP * pitch, LANES), jnp.float32),
            pltpu.SMEM((1,), jnp.int32),
        ],
        compiler_params=pltpu.CompilerParams(vmem_limit_bytes=VMEM_LIMIT),
        cost_estimate=pl.CostEstimate(flops=200_000_000, bytes_accessed=12_000_000, transcendentals=0),
        name="lay_out",
    )(slots, filled, held)


BATCH = 2


def encode_kernel(raw_ref, codes_ref, steps_ref, error_ref, codes, inverse, out_sems):
    sources, cap, flat = codes.shape
    lanes = inverse.shape[1]
    half = lanes // QUAD
    tiles = lanes // LANES
    batches = sources // BATCH

    def give(b):
        here = pl.ds(b * BATCH, BATCH)
        return pltpu.make_async_copy(codes.at[here], codes_ref.at[here], out_sems.at[b])

    peak = jnp.max(raw_ref[:, :, flat:].astype(jnp.float32), axis=0)
    scale = headroom * jnp.maximum(peak, 1.0) / 127.0
    rows = [jnp.broadcast_to(scale[n : n + 1], (cap, LANES)) for n in range(pl.cdiv(half, LANES))]
    for n, row in enumerate(rows):
        size = min(LANES, half - n * LANES)
        steps_ref[:, n * LANES : n * LANES + size] = row[:1, :size]
    for i, tile in enumerate(end_to_end([rows] * QUAD, half, 0)):
        inverse[:, i * LANES : (i + 1) * LANES] = 1.0 / tile
    by_lane = [inverse[:, i * LANES : (i + 1) * LANES] for i in range(tiles)]

    def batch(b, totals):
        def group(u, totals):
            totals = list(totals)
            for i in range(tiles):
                at = pl.ds(pl.multiple_of(u * lanes + i * LANES, LANES), LANES)
                for s in range(BATCH):
                    exact = raw_ref[b * BATCH + s, :, at].astype(jnp.float32) * by_lane[i]
                    coded = jnp.clip(exact, -127.0, 127.0).astype(jnp.bfloat16)
                    codes[b * BATCH + s, :, at] = coded
                    miss = exact - coded.astype(jnp.float32)
                    totals[i] = totals[i] + miss * miss
            return tuple(totals)

        totals = lax.fori_loop(0, flat // lanes, group, totals, unroll=4)
        give(b).start()
        return totals

    totals = lax.fori_loop(
        0, batches, batch, tuple(jnp.zeros((cap, LANES), jnp.float32) for _ in range(tiles))
    )
    whole = jnp.concatenate([jnp.sum(t, axis=0, keepdims=True) for t in totals], axis=1)
    error = whole[:, :half]
    for q in range(1, QUAD):
        error = error + whole[:, q * half : (q + 1) * half]
    error_ref[...] = error
    for b in range(batches):
        give(b).wait()


def encode(raw, half):
    sources, cap, size = raw.shape
    flat = size - LANES
    vmem = pl.BlockSpec(memory_space=pltpu.VMEM)
    return pl.pallas_call(
        encode_kernel,
        out_shape=[
            jax.ShapeDtypeStruct((sources, cap, flat), jnp.bfloat16),
            jax.ShapeDtypeStruct((1, half), jnp.float32),
            pltpu.VMEM((1, half), jnp.float32),
        ],
        in_specs=[vmem],
        out_specs=[pl.BlockSpec(memory_space=pltpu.HBM), vmem, vmem],
        scratch_shapes=[
            pltpu.VMEM((sources, cap, flat), jnp.bfloat16),
            pltpu.VMEM((cap, QUAD * half), jnp.float32),
            pltpu.SemaphoreType.DMA((sources // BATCH,)),
        ],
        compiler_params=pltpu.CompilerParams(vmem_limit_bytes=VMEM_LIMIT),
        cost_estimate=pl.CostEstimate(flops=80_000_000, bytes_accessed=19_000_000, transcendentals=0),
        name="encode",
    )(raw)


NEIGHBOURS = ([(0, 1), (1, 0), (2, 3), (3, 2)], [(0, 3), (3, 0), (1, 2), (2, 1)])


def body(block_pool, sel_index, sel_layer, counts):
    own_count = lax.axis_size("own")
    rep_count = lax.axis_size("rep")
    layers = own_count // SLICES
    tokens, width = block_pool.shape[1:]
    half = width // SLICES
    peak, *found = local_peaks(block_pool, sel_index, sel_layer, counts, layers)
    others = [lax.ppermute(peak, "rep", [(r, (r + k) % rep_count) for r in range(rep_count)]) for k in range(1, rep_count)]
    sent = lay_out(*found)
    peak = functools.reduce(jnp.maximum, others, peak)
    sent = lax.dynamic_update_slice(sent, peak, (0, 0, tokens * half))
    arrived = lax.all_to_all(sent, "own", split_axis=0, concat_axis=0, tiled=True)

    codes, steps, error = encode(arrived, half)
    for pairs in NEIGHBOURS:
        error = error + lax.ppermute(error, "rep", pairs)
    denominator = float(own_count * rep_count * CAP * tokens)
    return codes[None, None], steps, error / denominator


def solution(mesh):
    return jax.shard_map(
        body,
        mesh=mesh,
        in_specs=(
            P(("own", "rep"), None, None),
            P(("own", "rep")),
            P(("own", "rep")),
            P(("own", "rep")),
        ),
        out_specs=(P("own", "rep", None, None, None), P("own", None), P("own", None)),
        check_vma=False,
    )
```

```python
import functools
import jax
import jax.numpy as jnp
from jax import lax
from jax.experimental import pallas as pl
from jax.experimental.pallas import tpu as pltpu
from jax.sharding import PartitionSpec as P

SLICES = 2
CAP = 8
LANES = 128
QUAD = 4
headroom = 0.5
VMEM_LIMIT = 30 * 2**20


def end_to_end(rows, width, start):
    lane = lax.broadcasted_iota(jnp.int32, rows[0][0].shape, 1)
    turned, out = {}, []
    for i in range(len(rows) * width // LANES):
        whole, at = None, 0
        while at < LANES:
            flat = i * LANES + at
            q = flat // width
            source = flat - q * width + start
            j = source // LANES
            run = min(LANES - source % LANES, (q + 1) * width - flat, LANES - at)
            if (q, j) not in turned:
                shift = (at - source) % LANES
                turned[q, j] = pltpu.roll(rows[q][j], shift, 1) if shift else rows[q][j]
            piece = turned[q, j]
            whole = piece if whole is None else jnp.where(lane >= at, piece, whole)
            at += run
        out.append(whole)
    return out


def peak_kernel(index_ref, layer_ref, count_ref, pool_ref, out_ref, held, slots, filled, acc, top, sems):
    live = count_ref[0]
    tokens, width = held.shape[1:]
    layers = acc.shape[0]
    half = width // SLICES
    pieces = top.shape[0] // SLICES

    def fetch(j):
        return pltpu.make_async_copy(pool_ref.at[index_ref[j]], held.at[j], sems.at[j])

    for layer in range(layers):
        filled[layer] = 0

    def start(j, carry):
        fetch(j).start()
        layer = layer_ref[j]
        at = filled[layer]
        slots[layer * CAP + at] = j
        filled[layer] = at + 1
        return carry

    lax.fori_loop(0, live, start, 0)
    acc[...] = jnp.zeros_like(acc)
    top[...] = jnp.zeros_like(top)

    def wait(j, carry):
        fetch(j).wait()
        layer = layer_ref[j]
        values = jnp.abs(held[j].astype(jnp.float32)).reshape(tokens // 8, 8, width)
        acc[layer] = jnp.maximum(acc[layer], jnp.max(values, axis=0))
        return carry

    lax.fori_loop(0, live, wait, 0)
    whole = jnp.max(acc[...], axis=1)
    for h in range(SLICES):
        for n in range(pieces):
            lanes = min(LANES, half - n * LANES)
            at = h * half + n * LANES
            top[h * pieces + n, :, :lanes] = whole[:, at : at + lanes]
    row = lax.broadcasted_iota(jnp.int32, (CAP, LANES), 0)

    def tiles(layer, carry):
        for h in range(SLICES):
            tile = jnp.zeros((CAP, LANES), jnp.float32)
            for n in range(pieces):
                one = jnp.broadcast_to(top[h * pieces + n, pl.ds(layer, 1), :], (CAP, LANES))
                tile = jnp.where(row == n, one, tile)
            out_ref[layer * SLICES + h] = tile.astype(jnp.bfloat16)
        return carry

    lax.fori_loop(0, layers, tiles, 0, unroll=4)


def local_peaks(block_pool, sel_index, sel_layer, counts, layers):
    n_select = sel_index.shape[0]
    tokens, width = block_pool.shape[1:]
    pieces = pl.cdiv(width // SLICES, LANES)
    smem = pl.BlockSpec(memory_space=pltpu.SMEM)
    vmem = pl.BlockSpec(memory_space=pltpu.VMEM)
    return pl.pallas_call(
        peak_kernel,
        out_shape=[
            pltpu.VMEM((layers * SLICES, CAP, LANES), jnp.bfloat16),
            pltpu.VMEM((n_select, tokens, width), jnp.bfloat16),
            pltpu.SMEM((layers * CAP,), jnp.int32),
            pltpu.SMEM((layers,), jnp.int32),
        ],
        in_specs=[smem, smem, smem, pl.BlockSpec(memory_space=pltpu.HBM)],
        out_specs=[vmem, vmem, smem, smem],
        scratch_shapes=[
            pltpu.VMEM((layers, 8, width), jnp.float32),
            pltpu.VMEM((SLICES * pieces, layers, LANES), jnp.float32),
            pltpu.SemaphoreType.DMA((n_select,)),
        ],
        compiler_params=pltpu.CompilerParams(vmem_limit_bytes=2 * VMEM_LIMIT),
        cost_estimate=pl.CostEstimate(flops=20_000_000, bytes_accessed=2_500_000, transcendentals=0),
        name="peaks",
    )(sel_index, sel_layer, counts, block_pool)


def lay_out_kernel(slots, filled, held, built, spread, dirty):
    layers = filled.shape[0]
    tokens, width = held.shape[1:]
    half = width // SLICES
    tiles = spread.shape[0]
    pitch = spread.shape[1] // (CAP + 1)
    group = QUAD * half
    dirty[0] = CAP

    def build(layer, carry):
        held_slots = filled[layer]

        @pl.when(held_slots == 0)
        def _():
            built[pl.ds(SLICES * layer, SLICES), :, : tokens * half] = jnp.zeros(
                (SLICES, CAP, tokens * half), built.dtype
            )

        @pl.when(held_slots > 0)
        def _():
            def place(c, carry):
                values = held[slots[layer * CAP + c]].astype(jnp.float32)
                rows = pl.ds(c * pitch, tokens)
                for i in range(tiles):
                    lanes = min(LANES, width - i * LANES)
                    spread[i, rows, :lanes] = values[:, i * LANES : i * LANES + lanes]
                return carry

            lax.fori_loop(0, held_slots, place, 0)

            def blank(c, carry):
                for i in range(tiles):
                    spread[i, pl.ds(c * pitch, tokens), :] = jnp.zeros((tokens, LANES), jnp.float32)
                return carry

            lax.fori_loop(held_slots, dirty[0], blank, 0)
            dirty[0] = held_slots

            def four_tokens(u, carry):
                rows = [
                    [spread[i, pl.ds(QUAD * u + q, CAP, stride=pitch), :] for i in range(tiles)] for q in range(QUAD)
                ]
                for h in range(SLICES):
                    for i, tile in enumerate(end_to_end(rows, half, h * half)):
                        where = pl.ds(pl.multiple_of(u * group + i * LANES, LANES), LANES)
                        built[SLICES * layer + h, :, where] = tile.astype(jnp.bfloat16)
                return carry

            lax.fori_loop(0, tokens // QUAD, four_tokens, 0, unroll=tokens // QUAD)

        return carry

    lax.fori_loop(0, layers, build, 0)


def lay_out(held, slots, filled):
    layers = filled.shape[0]
    _, tokens, width = held.shape
    flat = tokens * (width // SLICES)
    pitch = tokens + 1
    smem = pl.BlockSpec(memory_space=pltpu.SMEM)
    vmem = pl.BlockSpec(memory_space=pltpu.VMEM)
    return pl.pallas_call(
        lay_out_kernel,
        out_shape=pltpu.VMEM((layers * SLICES, CAP, flat + LANES), jnp.bfloat16),
        in_specs=[smem, smem, vmem],
        out_specs=vmem,
        scratch_shapes=[
            pltpu.VMEM((pl.cdiv(width, LANES), (CAP + 1) * pitch, LANES), jnp.float32),
            pltpu.SMEM((1,), jnp.int32),
        ],
        compiler_params=pltpu.CompilerParams(vmem_limit_bytes=VMEM_LIMIT),
        cost_estimate=pl.CostEstimate(flops=200_000_000, bytes_accessed=12_000_000, transcendentals=0),
        name="lay_out",
    )(slots, filled, held)


BATCH = 2


def encode_kernel(raw_ref, codes_ref, steps_ref, error_ref, codes, inverse, out_sems):
    sources, cap, flat = codes.shape
    lanes = inverse.shape[1]
    half = lanes // QUAD
    tiles = lanes // LANES
    batches = sources // BATCH

    def give(b):
        here = pl.ds(b * BATCH, BATCH)
        return pltpu.make_async_copy(codes.at[here], codes_ref.at[here], out_sems.at[b])

    peak = jnp.max(raw_ref[:, :, flat:].astype(jnp.float32), axis=0)
    scale = headroom * jnp.maximum(peak, 1.0) / 127.0
    rows = [jnp.broadcast_to(scale[n : n + 1], (cap, LANES)) for n in range(pl.cdiv(half, LANES))]
    for n, row in enumerate(rows):
        size = min(LANES, half - n * LANES)
        steps_ref[:, n * LANES : n * LANES + size] = row[:1, :size]
    for i, tile in enumerate(end_to_end([rows] * QUAD, half, 0)):
        inverse[:, i * LANES : (i + 1) * LANES] = 1.0 / tile
    by_lane = [inverse[:, i * LANES : (i + 1) * LANES] for i in range(tiles)]

    def batch(b, totals):
        def group(u, totals):
            totals = list(totals)
            for s in range(BATCH):
                for i in range(tiles):
                    at = pl.ds(pl.multiple_of(u * lanes + i * LANES, LANES), LANES)
                    exact = raw_ref[b * BATCH + s, :, at].astype(jnp.float32) * by_lane[i]
                    coded = jnp.clip(exact, -127.0, 127.0).astype(jnp.bfloat16)
                    codes[b * BATCH + s, :, at] = coded
                    miss = exact - coded.astype(jnp.float32)
                    totals[i] = totals[i] + miss * miss
            return tuple(totals)

        totals = lax.fori_loop(0, flat // lanes, group, totals, unroll=flat // lanes)
        give(b).start()
        return totals

    totals = lax.fori_loop(
        0, batches, batch, tuple(jnp.zeros((cap, LANES), jnp.float32) for _ in range(tiles))
    )
    whole = jnp.concatenate([jnp.sum(t, axis=0, keepdims=True) for t in totals], axis=1)
    error = whole[:, :half]
    for q in range(1, QUAD):
        error = error + whole[:, q * half : (q + 1) * half]
    error_ref[...] = error
    for b in range(batches):
        give(b).wait()


def encode(raw, half):
    sources, cap, size = raw.shape
    flat = size - LANES
    vmem = pl.BlockSpec(memory_space=pltpu.VMEM)
    return pl.pallas_call(
        encode_kernel,
        out_shape=[
            jax.ShapeDtypeStruct((sources, cap, flat), jnp.bfloat16),
            jax.ShapeDtypeStruct((1, half), jnp.float32),
            pltpu.VMEM((1, half), jnp.float32),
        ],
        in_specs=[vmem],
        out_specs=[pl.BlockSpec(memory_space=pltpu.HBM), vmem, vmem],
        scratch_shapes=[
            pltpu.VMEM((sources, cap, flat), jnp.bfloat16),
            pltpu.VMEM((cap, QUAD * half), jnp.float32),
            pltpu.SemaphoreType.DMA((sources // BATCH,)),
        ],
        compiler_params=pltpu.CompilerParams(vmem_limit_bytes=VMEM_LIMIT),
        cost_estimate=pl.CostEstimate(flops=80_000_000, bytes_accessed=19_000_000, transcendentals=0),
        name="encode",
    )(raw)


def from_others(x, axis):
    count = lax.axis_size(axis)
    return [lax.ppermute(x, axis, [(r, (r + k) % count) for r in range(count)]) for k in range(1, count)]


def body(block_pool, sel_index, sel_layer, counts):
    own_count = lax.axis_size("own")
    rep_count = lax.axis_size("rep")
    layers = own_count // SLICES
    tokens, width = block_pool.shape[1:]
    half = width // SLICES
    peak, *found = local_peaks(block_pool, sel_index, sel_layer, counts, layers)
    others = from_others(peak, "rep")
    sent = lay_out(*found)
    peak = functools.reduce(jnp.maximum, others, peak)
    sent = lax.dynamic_update_slice(sent, peak, (0, 0, tokens * half))
    arrived = lax.all_to_all(sent, "own", split_axis=0, concat_axis=0, tiled=True)

    codes, steps, error = encode(arrived, half)
    error = functools.reduce(jnp.add, from_others(error, "rep"), error)
    denominator = float(own_count * rep_count * CAP * tokens)
    return codes[None, None], steps, error / denominator


def solution(mesh):
    return jax.shard_map(
        body,
        mesh=mesh,
        in_specs=(
            P(("own", "rep"), None, None),
            P(("own", "rep")),
            P(("own", "rep")),
            P(("own", "rep")),
        ),
        out_specs=(P("own", "rep", None, None, None), P("own", None), P("own", None)),
        check_vma=False,
    )
```

```python
import functools
import jax
import jax.numpy as jnp
from jax import lax
from jax.experimental import pallas as pl
from jax.experimental.pallas import tpu as pltpu
from jax.sharding import PartitionSpec as P

SLICES = 2
CAP = 8
LANES = 128
QUAD = 4
headroom = 0.5
VMEM_LIMIT = 30 * 2**20


def end_to_end(rows, width, start):
    lane = lax.broadcasted_iota(jnp.int32, rows[0][0].shape, 1)
    turned, out = {}, []
    for i in range(len(rows) * width // LANES):
        whole, at = None, 0
        while at < LANES:
            flat = i * LANES + at
            q = flat // width
            source = flat - q * width + start
            j = source // LANES
            run = min(LANES - source % LANES, (q + 1) * width - flat, LANES - at)
            if (q, j) not in turned:
                shift = (at - source) % LANES
                turned[q, j] = pltpu.roll(rows[q][j], shift, 1) if shift else rows[q][j]
            piece = turned[q, j]
            whole = piece if whole is None else jnp.where(lane >= at, piece, whole)
            at += run
        out.append(whole)
    return out


def peak_kernel(index_ref, layer_ref, count_ref, pool_ref, out_ref, held, slots, filled, acc, top, sems):
    live = count_ref[0]
    tokens, width = held.shape[1:]
    layers = acc.shape[0]
    half = width // SLICES
    pieces = top.shape[0] // SLICES

    def fetch(j):
        return pltpu.make_async_copy(pool_ref.at[index_ref[j]], held.at[j], sems.at[j])

    for layer in range(layers):
        filled[layer] = 0

    def start(j, carry):
        fetch(j).start()
        layer = layer_ref[j]
        at = filled[layer]
        slots[layer * CAP + at] = j
        filled[layer] = at + 1
        return carry

    lax.fori_loop(0, live, start, 0)
    acc[...] = jnp.zeros_like(acc)
    top[...] = jnp.zeros_like(top)

    def wait(j, carry):
        fetch(j).wait()
        layer = layer_ref[j]
        values = jnp.abs(held[j].astype(jnp.float32)).reshape(tokens // 8, 8, width)
        acc[layer] = jnp.maximum(acc[layer], jnp.max(values, axis=0))
        return carry

    lax.fori_loop(0, live, wait, 0)
    whole = jnp.max(acc[...], axis=1)
    for h in range(SLICES):
        for n in range(pieces):
            lanes = min(LANES, half - n * LANES)
            at = h * half + n * LANES
            top[h * pieces + n, :, :lanes] = whole[:, at : at + lanes]
    row = lax.broadcasted_iota(jnp.int32, (CAP, LANES), 0)

    def tiles(layer, carry):
        for h in range(SLICES):
            tile = jnp.zeros((CAP, LANES), jnp.float32)
            for n in range(pieces):
                one = jnp.broadcast_to(top[h * pieces + n, pl.ds(layer, 1), :], (CAP, LANES))
                tile = jnp.where(row == n, one, tile)
            out_ref[layer * SLICES + h] = tile.astype(jnp.bfloat16)
        return carry

    lax.fori_loop(0, layers, tiles, 0, unroll=4)


def local_peaks(block_pool, sel_index, sel_layer, counts, layers):
    n_select = sel_index.shape[0]
    tokens, width = block_pool.shape[1:]
    pieces = pl.cdiv(width // SLICES, LANES)
    smem = pl.BlockSpec(memory_space=pltpu.SMEM)
    vmem = pl.BlockSpec(memory_space=pltpu.VMEM)
    return pl.pallas_call(
        peak_kernel,
        out_shape=[
            pltpu.VMEM((layers * SLICES, CAP, LANES), jnp.bfloat16),
            pltpu.VMEM((n_select, tokens, width), jnp.bfloat16),
            pltpu.SMEM((layers * CAP,), jnp.int32),
            pltpu.SMEM((layers,), jnp.int32),
        ],
        in_specs=[smem, smem, smem, pl.BlockSpec(memory_space=pltpu.HBM)],
        out_specs=[vmem, vmem, smem, smem],
        scratch_shapes=[
            pltpu.VMEM((layers, 8, width), jnp.float32),
            pltpu.VMEM((SLICES * pieces, layers, LANES), jnp.float32),
            pltpu.SemaphoreType.DMA((n_select,)),
        ],
        compiler_params=pltpu.CompilerParams(vmem_limit_bytes=2 * VMEM_LIMIT),
        cost_estimate=pl.CostEstimate(flops=20_000_000, bytes_accessed=2_500_000, transcendentals=0),
        name="peaks",
    )(sel_index, sel_layer, counts, block_pool)


def lay_out_kernel(slots, filled, held, built, spread, dirty):
    layers = filled.shape[0]
    tokens, width = held.shape[1:]
    half = width // SLICES
    tiles = spread.shape[0]
    pitch = spread.shape[1] // (CAP + 1)
    group = QUAD * half
    dirty[0] = CAP

    def build(layer, carry):
        held_slots = filled[layer]

        @pl.when(held_slots == 0)
        def _():
            built[pl.ds(SLICES * layer, SLICES), :, : tokens * half] = jnp.zeros(
                (SLICES, CAP, tokens * half), built.dtype
            )

        @pl.when(held_slots > 0)
        def _():
            def place(c, carry):
                values = held[slots[layer * CAP + c]].astype(jnp.float32)
                rows = pl.ds(c * pitch, tokens)
                for i in range(tiles):
                    lanes = min(LANES, width - i * LANES)
                    spread[i, rows, :lanes] = values[:, i * LANES : i * LANES + lanes]
                return carry

            lax.fori_loop(0, held_slots, place, 0)

            def blank(c, carry):
                for i in range(tiles):
                    spread[i, pl.ds(c * pitch, tokens), :] = jnp.zeros((tokens, LANES), jnp.float32)
                return carry

            lax.fori_loop(held_slots, dirty[0], blank, 0)
            dirty[0] = held_slots

            def four_tokens(u, carry):
                rows = [
                    [spread[i, pl.ds(QUAD * u + q, CAP, stride=pitch), :] for i in range(tiles)] for q in range(QUAD)
                ]
                for h in range(SLICES):
                    for i, tile in enumerate(end_to_end(rows, half, h * half)):
                        where = pl.ds(pl.multiple_of(u * group + i * LANES, LANES), LANES)
                        built[SLICES * layer + h, :, where] = tile.astype(jnp.bfloat16)
                return carry

            lax.fori_loop(0, tokens // QUAD, four_tokens, 0, unroll=tokens // QUAD)

        return carry

    lax.fori_loop(0, layers, build, 0)


def lay_out(held, slots, filled):
    layers = filled.shape[0]
    _, tokens, width = held.shape
    flat = tokens * (width // SLICES)
    pitch = tokens + 1
    smem = pl.BlockSpec(memory_space=pltpu.SMEM)
    vmem = pl.BlockSpec(memory_space=pltpu.VMEM)
    return pl.pallas_call(
        lay_out_kernel,
        out_shape=pltpu.VMEM((layers * SLICES, CAP, flat + LANES), jnp.bfloat16),
        in_specs=[smem, smem, vmem],
        out_specs=vmem,
        scratch_shapes=[
            pltpu.VMEM((pl.cdiv(width, LANES), (CAP + 1) * pitch, LANES), jnp.float32),
            pltpu.SMEM((1,), jnp.int32),
        ],
        compiler_params=pltpu.CompilerParams(vmem_limit_bytes=VMEM_LIMIT),
        cost_estimate=pl.CostEstimate(flops=200_000_000, bytes_accessed=12_000_000, transcendentals=0),
        name="lay_out",
    )(slots, filled, held)


BATCH = 2


def encode_kernel(raw_ref, codes_ref, steps_ref, error_ref, inverse, codes, out_sems):
    sources = raw_ref.shape[0]
    first, cap, flat = codes.shape
    lanes = inverse.shape[1]
    half = lanes // QUAD
    tiles = lanes // LANES
    batches = sources // BATCH

    def give(b):
        here = pl.ds(b * BATCH, BATCH)
        return pltpu.make_async_copy(codes.at[here], codes_ref.at[here], out_sems.at[b])

    peak = jnp.max(raw_ref[:, :, flat:].astype(jnp.float32), axis=0)
    scale = headroom * jnp.maximum(peak, 1.0) / 127.0
    rows = [jnp.broadcast_to(scale[n : n + 1], (cap, LANES)) for n in range(pl.cdiv(half, LANES))]
    for n, row in enumerate(rows):
        size = min(LANES, half - n * LANES)
        steps_ref[:, n * LANES : n * LANES + size] = row[:1, :size]
    for i, tile in enumerate(end_to_end([rows] * QUAD, half, 0)):
        inverse[:, i * LANES : (i + 1) * LANES] = 1.0 / tile
    by_lane = [inverse[:, i * LANES : (i + 1) * LANES] for i in range(tiles)]

    def batch(b, totals, coding):
        def group(u, totals):
            totals = list(totals)
            for s in range(BATCH):
                for i in range(tiles):
                    at = pl.ds(pl.multiple_of(u * lanes + i * LANES, LANES), LANES)
                    exact = raw_ref[b * BATCH + s, :, at].astype(jnp.float32) * by_lane[i]
                    coded = jnp.clip(exact, -127.0, 127.0).astype(jnp.bfloat16)
                    if coding:
                        codes[b * BATCH + s, :, at] = coded
                    miss = exact - coded.astype(jnp.float32)
                    totals[i] = totals[i] + miss * miss
            return tuple(totals)

        totals = lax.fori_loop(0, flat // lanes, group, totals, unroll=flat // lanes)
        if coding:
            give(b).start()
        return totals

    totals = tuple(jnp.zeros((cap, LANES), jnp.float32) for _ in range(tiles))
    totals = lax.fori_loop(0, first // BATCH, functools.partial(batch, coding=True), totals)
    totals = lax.fori_loop(first // BATCH, batches, functools.partial(batch, coding=False), totals)
    whole = jnp.concatenate([jnp.sum(t, axis=0, keepdims=True) for t in totals], axis=1)
    error = whole[:, :half]
    for q in range(1, QUAD):
        error = error + whole[:, q * half : (q + 1) * half]
    error_ref[...] = error
    for b in range(first // BATCH):
        give(b).wait()


def encode(raw, half, first):
    sources, cap, size = raw.shape
    flat = size - LANES
    vmem = pl.BlockSpec(memory_space=pltpu.VMEM)
    return pl.pallas_call(
        encode_kernel,
        out_shape=[
            jax.ShapeDtypeStruct((sources, cap, flat), jnp.bfloat16),
            jax.ShapeDtypeStruct((1, half), jnp.float32),
            pltpu.VMEM((1, half), jnp.float32),
            pltpu.VMEM((cap, QUAD * half), jnp.float32),
        ],
        in_specs=[vmem],
        out_specs=[pl.BlockSpec(memory_space=pltpu.HBM), vmem, vmem, vmem],
        scratch_shapes=[
            pltpu.VMEM((first, cap, flat), jnp.bfloat16),
            pltpu.SemaphoreType.DMA((first // BATCH,)),
        ],
        compiler_params=pltpu.CompilerParams(vmem_limit_bytes=VMEM_LIMIT),
        cost_estimate=pl.CostEstimate(flops=80_000_000, bytes_accessed=19_000_000, transcendentals=0),
        name="encode",
    )(raw)


def encode_rest_kernel(raw_ref, inverse, _, codes_ref, codes, out_sems):
    count, _, flat = codes.shape
    first = raw_ref.shape[0] - count
    lanes = inverse.shape[1]
    by_lane = [inverse[:, i : i + LANES] for i in range(0, lanes, LANES)]

    def give(b):
        here = pl.ds(b * BATCH, BATCH)
        return pltpu.make_async_copy(codes.at[here], codes_ref.at[pl.ds(first + b * BATCH, BATCH)], out_sems.at[b])

    def batch(b, carry):
        for s in range(BATCH):
            for i in range(flat // LANES):
                at = slice(i * LANES, (i + 1) * LANES)
                exact = raw_ref[first + b * BATCH + s, :, at].astype(jnp.float32) * by_lane[i % len(by_lane)]
                codes[b * BATCH + s, :, at] = jnp.clip(exact, -127.0, 127.0).astype(jnp.bfloat16)
        give(b).start()
        return carry

    lax.fori_loop(0, count // BATCH, batch, 0)
    for b in range(count // BATCH):
        give(b).wait()


def encode_rest(raw, inverse, codes, first):
    rest = raw.shape[0] - first
    vmem = pl.BlockSpec(memory_space=pltpu.VMEM)
    hbm = pl.BlockSpec(memory_space=pltpu.HBM)
    return pl.pallas_call(
        encode_rest_kernel,
        out_shape=jax.ShapeDtypeStruct(codes.shape, codes.dtype),
        in_specs=[vmem, vmem, hbm],
        out_specs=hbm,
        scratch_shapes=[
            pltpu.VMEM((rest, *codes.shape[1:]), codes.dtype),
            pltpu.SemaphoreType.DMA((rest // BATCH,)),
        ],
        input_output_aliases={2: 0},
        compiler_params=pltpu.CompilerParams(vmem_limit_bytes=VMEM_LIMIT),
        cost_estimate=pl.CostEstimate(flops=200_000_000, bytes_accessed=5_000_000, transcendentals=0),
        name="encode_rest",
    )(raw, inverse, codes)


def from_others(x, axis):
    count = lax.axis_size(axis)
    return [lax.ppermute(x, axis, [(r, (r + k) % count) for r in range(count)]) for k in range(1, count)]


def body(block_pool, sel_index, sel_layer, counts):
    own_count = lax.axis_size("own")
    rep_count = lax.axis_size("rep")
    layers = own_count // SLICES
    tokens, width = block_pool.shape[1:]
    half = width // SLICES
    peak, *found = local_peaks(block_pool, sel_index, sel_layer, counts, layers)
    others = from_others(peak, "rep")
    sent = lay_out(*found)
    peak = functools.reduce(jnp.maximum, others, peak)
    sent = lax.dynamic_update_slice(sent, peak, (0, 0, tokens * half))
    arrived = lax.all_to_all(sent, "own", split_axis=0, concat_axis=0, tiled=True)

    first = own_count * 3 // 4
    codes, steps, error, inverse = encode(arrived, half, first)
    others = from_others(error, "rep")
    codes = encode_rest(arrived, inverse, codes, first)
    error = functools.reduce(jnp.add, others, error)
    denominator = float(own_count * rep_count * CAP * tokens)
    return codes[None, None], steps, error / denominator


def solution(mesh):
    return jax.shard_map(
        body,
        mesh=mesh,
        in_specs=(
            P(("own", "rep"), None, None),
            P(("own", "rep")),
            P(("own", "rep")),
            P(("own", "rep")),
        ),
        out_specs=(P("own", "rep", None, None, None), P("own", None), P("own", None)),
        check_vma=False,
    )
```

```python
import functools
import jax
import jax.numpy as jnp
from jax import lax
from jax.experimental import pallas as pl
from jax.experimental.pallas import tpu as pltpu
from jax.sharding import PartitionSpec as P

SLICES = 2
CAP = 8
LANES = 128
QUAD = 4
headroom = 0.5
VMEM_LIMIT = 30 * 2**20


def end_to_end(rows, width, start):
    lane = lax.broadcasted_iota(jnp.int32, rows[0][0].shape, 1)
    turned, out = {}, []
    for i in range(len(rows) * width // LANES):
        whole, at = None, 0
        while at < LANES:
            flat = i * LANES + at
            q = flat // width
            source = flat - q * width + start
            j = source // LANES
            run = min(LANES - source % LANES, (q + 1) * width - flat, LANES - at)
            if (q, j) not in turned:
                shift = (at - source) % LANES
                turned[q, j] = pltpu.roll(rows[q][j], shift, 1) if shift else rows[q][j]
            piece = turned[q, j]
            whole = piece if whole is None else jnp.where(lane >= at, piece, whole)
            at += run
        out.append(whole)
    return out


def peak_kernel(index_ref, layer_ref, count_ref, pool_ref, out_ref, held, slots, filled, acc, top, sems):
    live = count_ref[0]
    tokens, width = held.shape[1:]
    layers = acc.shape[0]
    half = width // SLICES
    pieces = top.shape[0] // SLICES

    def fetch(j):
        return pltpu.make_async_copy(pool_ref.at[index_ref[j]], held.at[j], sems.at[j])

    for layer in range(layers):
        filled[layer] = 0

    def start(j, carry):
        fetch(j).start()
        layer = layer_ref[j]
        at = filled[layer]
        slots[layer * CAP + at] = j
        filled[layer] = at + 1
        return carry

    lax.fori_loop(0, live, start, 0)
    acc[...] = jnp.zeros_like(acc)
    top[...] = jnp.zeros_like(top)

    def wait(j, carry):
        fetch(j).wait()
        layer = layer_ref[j]
        values = jnp.abs(held[j].astype(jnp.float32)).reshape(tokens // 8, 8, width)
        acc[layer] = jnp.maximum(acc[layer], jnp.max(values, axis=0))
        return carry

    lax.fori_loop(0, live, wait, 0)
    whole = jnp.max(acc[...], axis=1)
    for h in range(SLICES):
        for n in range(pieces):
            lanes = min(LANES, half - n * LANES)
            at = h * half + n * LANES
            top[h * pieces + n, :, :lanes] = whole[:, at : at + lanes]
    row = lax.broadcasted_iota(jnp.int32, (CAP, LANES), 0)

    def tiles(layer, carry):
        for h in range(SLICES):
            tile = jnp.zeros((CAP, LANES), jnp.float32)
            for n in range(pieces):
                one = jnp.broadcast_to(top[h * pieces + n, pl.ds(layer, 1), :], (CAP, LANES))
                tile = jnp.where(row == n, one, tile)
            out_ref[layer * SLICES + h] = tile.astype(jnp.bfloat16)
        return carry

    lax.fori_loop(0, layers, tiles, 0, unroll=4)


def local_peaks(block_pool, sel_index, sel_layer, counts, layers):
    n_select = sel_index.shape[0]
    tokens, width = block_pool.shape[1:]
    pieces = pl.cdiv(width // SLICES, LANES)
    smem = pl.BlockSpec(memory_space=pltpu.SMEM)
    vmem = pl.BlockSpec(memory_space=pltpu.VMEM)
    return pl.pallas_call(
        peak_kernel,
        out_shape=[
            pltpu.VMEM((layers * SLICES, CAP, LANES), jnp.bfloat16),
            pltpu.VMEM((n_select, tokens, width), jnp.bfloat16),
            pltpu.SMEM((layers * CAP,), jnp.int32),
            pltpu.SMEM((layers,), jnp.int32),
        ],
        in_specs=[smem, smem, smem, pl.BlockSpec(memory_space=pltpu.HBM)],
        out_specs=[vmem, vmem, smem, smem],
        scratch_shapes=[
            pltpu.VMEM((layers, 8, width), jnp.float32),
            pltpu.VMEM((SLICES * pieces, layers, LANES), jnp.float32),
            pltpu.SemaphoreType.DMA((n_select,)),
        ],
        compiler_params=pltpu.CompilerParams(vmem_limit_bytes=2 * VMEM_LIMIT),
        cost_estimate=pl.CostEstimate(flops=20_000_000, bytes_accessed=2_500_000, transcendentals=0),
        name="peaks",
    )(sel_index, sel_layer, counts, block_pool)


def lay_out_kernel(slots, filled, held, built, spread, dirty):
    layers = filled.shape[0]
    tokens, width = held.shape[1:]
    half = width // SLICES
    tiles = spread.shape[0]
    pitch = spread.shape[1] // (CAP + 1)
    group = QUAD * half
    dirty[0] = CAP

    def build(layer, carry):
        held_slots = filled[layer]

        @pl.when(held_slots == 0)
        def _():
            built[pl.ds(SLICES * layer, SLICES), :, : tokens * half] = jnp.zeros(
                (SLICES, CAP, tokens * half), built.dtype
            )

        @pl.when(held_slots > 0)
        def _():
            def place(c, carry):
                values = held[slots[layer * CAP + c]].astype(jnp.float32)
                rows = pl.ds(c * pitch, tokens)
                for i in range(tiles):
                    lanes = min(LANES, width - i * LANES)
                    spread[i, rows, :lanes] = values[:, i * LANES : i * LANES + lanes]
                return carry

            lax.fori_loop(0, held_slots, place, 0)

            def blank(c, carry):
                for i in range(tiles):
                    spread[i, pl.ds(c * pitch, tokens), :] = jnp.zeros((tokens, LANES), jnp.float32)
                return carry

            lax.fori_loop(held_slots, dirty[0], blank, 0)
            dirty[0] = held_slots

            def four_tokens(u, carry):
                rows = [
                    [spread[i, pl.ds(QUAD * u + q, CAP, stride=pitch), :] for i in range(tiles)] for q in range(QUAD)
                ]
                for h in range(SLICES):
                    for i, tile in enumerate(end_to_end(rows, half, h * half)):
                        where = pl.ds(pl.multiple_of(u * group + i * LANES, LANES), LANES)
                        built[SLICES * layer + h, :, where] = tile.astype(jnp.bfloat16)
                return carry

            lax.fori_loop(0, tokens // QUAD, four_tokens, 0, unroll=tokens // QUAD)

        return carry

    lax.fori_loop(0, layers, build, 0)


def lay_out(held, slots, filled):
    layers = filled.shape[0]
    _, tokens, width = held.shape
    flat = tokens * (width // SLICES)
    pitch = tokens + 1
    smem = pl.BlockSpec(memory_space=pltpu.SMEM)
    vmem = pl.BlockSpec(memory_space=pltpu.VMEM)
    return pl.pallas_call(
        lay_out_kernel,
        out_shape=pltpu.VMEM((layers * SLICES, CAP, flat + LANES), jnp.bfloat16),
        in_specs=[smem, smem, vmem],
        out_specs=vmem,
        scratch_shapes=[
            pltpu.VMEM((pl.cdiv(width, LANES), (CAP + 1) * pitch, LANES), jnp.float32),
            pltpu.SMEM((1,), jnp.int32),
        ],
        compiler_params=pltpu.CompilerParams(vmem_limit_bytes=VMEM_LIMIT),
        cost_estimate=pl.CostEstimate(flops=200_000_000, bytes_accessed=12_000_000, transcendentals=0),
        name="lay_out",
    )(slots, filled, held)


BATCH = 2


def encode_kernel(raw_ref, codes_ref, steps_ref, error_ref, codes, inverse, out_sems):
    sources, cap, flat = codes.shape
    lanes = inverse.shape[1]
    half = lanes // QUAD
    tiles = lanes // LANES
    batches = sources // BATCH

    def give(b):
        here = pl.ds(b * BATCH, BATCH)
        return pltpu.make_async_copy(codes.at[here], codes_ref.at[here], out_sems.at[b])

    peak = jnp.max(raw_ref[:, :, flat:].astype(jnp.float32), axis=0)
    scale = headroom * jnp.maximum(peak, 1.0) / 127.0
    rows = [jnp.broadcast_to(scale[n : n + 1], (cap, LANES)) for n in range(pl.cdiv(half, LANES))]
    for n, row in enumerate(rows):
        size = min(LANES, half - n * LANES)
        steps_ref[:, n * LANES : n * LANES + size] = row[:1, :size]
    for i, tile in enumerate(end_to_end([rows] * QUAD, half, 0)):
        inverse[:, i * LANES : (i + 1) * LANES] = 1.0 / tile
    by_lane = [inverse[:, i * LANES : (i + 1) * LANES] for i in range(tiles)]

    def batch(b, totals):
        def group(u, totals):
            totals = list(totals)
            for s in range(BATCH):
                for i in range(tiles):
                    at = pl.ds(pl.multiple_of(u * lanes + i * LANES, LANES), LANES)
                    exact = raw_ref[b * BATCH + s, :, at].astype(jnp.float32) * by_lane[i]
                    coded = jnp.clip(exact, -127.0, 127.0).astype(jnp.bfloat16)
                    codes[b * BATCH + s, :, at] = coded
                    miss = exact - coded.astype(jnp.float32)
                    totals[i] = totals[i] + miss * miss
            return tuple(totals)

        totals = lax.fori_loop(0, flat // lanes, group, totals, unroll=flat // lanes)
        give(b).start()
        return totals

    totals = lax.fori_loop(
        0, batches, batch, tuple(jnp.zeros((cap, LANES), jnp.float32) for _ in range(tiles))
    )
    whole = jnp.concatenate([jnp.sum(t, axis=0, keepdims=True) for t in totals], axis=1)
    error = whole[:, :half]
    for q in range(1, QUAD):
        error = error + whole[:, q * half : (q + 1) * half]
    error_ref[...] = error
    for b in range(batches):
        give(b).wait()


def encode(raw, half):
    sources, cap, size = raw.shape
    flat = size - LANES
    vmem = pl.BlockSpec(memory_space=pltpu.VMEM)
    return pl.pallas_call(
        encode_kernel,
        out_shape=[
            jax.ShapeDtypeStruct((sources, cap, flat), jnp.bfloat16),
            jax.ShapeDtypeStruct((1, half), jnp.float32),
            pltpu.VMEM((1, half), jnp.float32),
        ],
        in_specs=[vmem],
        out_specs=[pl.BlockSpec(memory_space=pltpu.HBM), vmem, vmem],
        scratch_shapes=[
            pltpu.VMEM((sources, cap, flat), jnp.bfloat16),
            pltpu.VMEM((cap, QUAD * half), jnp.float32),
            pltpu.SemaphoreType.DMA((sources // BATCH,)),
        ],
        compiler_params=pltpu.CompilerParams(vmem_limit_bytes=VMEM_LIMIT),
        cost_estimate=pl.CostEstimate(flops=80_000_000, bytes_accessed=19_000_000, transcendentals=0),
        name="encode",
    )(raw)


def from_others(x, axis):
    count = lax.axis_size(axis)
    hops = sorted(range(1, count), key=lambda k: min(k, count - k))
    return [lax.ppermute(x, axis, [(r, (r + k) % count) for r in range(count)]) for k in hops]


def body(block_pool, sel_index, sel_layer, counts):
    own_count = lax.axis_size("own")
    rep_count = lax.axis_size("rep")
    layers = own_count // SLICES
    tokens, width = block_pool.shape[1:]
    half = width // SLICES
    peak, *found = local_peaks(block_pool, sel_index, sel_layer, counts, layers)
    others = from_others(peak, "rep")
    sent = lay_out(*found)
    peak = functools.reduce(jnp.maximum, others, peak)
    sent = lax.dynamic_update_slice(sent, peak, (0, 0, tokens * half))
    arrived = lax.all_to_all(sent, "own", split_axis=0, concat_axis=0, tiled=True)

    codes, steps, error = encode(arrived, half)
    error = functools.reduce(jnp.add, from_others(error, "rep"), error)
    denominator = float(own_count * rep_count * CAP * tokens)
    return codes[None, None], steps, error / denominator


def solution(mesh):
    return jax.shard_map(
        body,
        mesh=mesh,
        in_specs=(
            P(("own", "rep"), None, None),
            P(("own", "rep")),
            P(("own", "rep")),
            P(("own", "rep")),
        ),
        out_specs=(P("own", "rep", None, None, None), P("own", None), P("own", None)),
        check_vma=False,
    )
```

```python
import functools
import jax
import jax.numpy as jnp
from jax import lax
from jax.experimental import pallas as pl
from jax.experimental.pallas import tpu as pltpu
from jax.sharding import PartitionSpec as P

SLICES = 2
CAP = 8
LANES = 128
QUAD = 4
headroom = 0.5
VMEM_LIMIT = 30 * 2**20


def end_to_end(rows, width, start):
    lane = lax.broadcasted_iota(jnp.int32, rows[0][0].shape, 1)
    turned, out = {}, []
    for i in range(len(rows) * width // LANES):
        whole, at = None, 0
        while at < LANES:
            flat = i * LANES + at
            q = flat // width
            source = flat - q * width + start
            j = source // LANES
            run = min(LANES - source % LANES, (q + 1) * width - flat, LANES - at)
            if (q, j) not in turned:
                shift = (at - source) % LANES
                turned[q, j] = pltpu.roll(rows[q][j], shift, 1) if shift else rows[q][j]
            piece = turned[q, j]
            whole = piece if whole is None else jnp.where(lane >= at, piece, whole)
            at += run
        out.append(whole)
    return out


def peak_kernel(index_ref, layer_ref, count_ref, pool_ref, out_ref, held, slots, filled, acc, top, sems):
    live = count_ref[0]
    tokens, width = held.shape[1:]
    layers = acc.shape[0]
    half = width // SLICES
    pieces = top.shape[0] // SLICES

    def fetch(j):
        return pltpu.make_async_copy(pool_ref.at[index_ref[j]], held.at[j], sems.at[j])

    for layer in range(layers):
        filled[layer] = 0

    def start(j, carry):
        fetch(j).start()
        layer = layer_ref[j]
        at = filled[layer]
        slots[layer * CAP + at] = j
        filled[layer] = at + 1
        return carry

    lax.fori_loop(0, live, start, 0)
    acc[...] = jnp.zeros_like(acc)
    top[...] = jnp.zeros_like(top)

    def wait(j, carry):
        fetch(j).wait()
        layer = layer_ref[j]
        values = jnp.abs(held[j])
        rows = tokens
        while rows > 16:
            rows //= 2
            values = jnp.maximum(values[:rows], values[rows:])
        values = values.astype(jnp.float32)
        acc[layer] = jnp.maximum(acc[layer], jnp.maximum(values[:8], values[8:]))
        return carry

    lax.fori_loop(0, live, wait, 0)
    whole = jnp.max(acc[...], axis=1)
    for h in range(SLICES):
        for n in range(pieces):
            lanes = min(LANES, half - n * LANES)
            at = h * half + n * LANES
            top[h * pieces + n, :, :lanes] = whole[:, at : at + lanes]
    row = lax.broadcasted_iota(jnp.int32, (CAP, LANES), 0)

    def tiles(layer, carry):
        for h in range(SLICES):
            tile = jnp.zeros((CAP, LANES), jnp.float32)
            for n in range(pieces):
                one = jnp.broadcast_to(top[h * pieces + n, pl.ds(layer, 1), :], (CAP, LANES))
                tile = jnp.where(row == n, one, tile)
            out_ref[layer * SLICES + h] = tile.astype(jnp.bfloat16)
        return carry

    lax.fori_loop(0, layers, tiles, 0, unroll=4)


def local_peaks(block_pool, sel_index, sel_layer, counts, layers):
    n_select = sel_index.shape[0]
    tokens, width = block_pool.shape[1:]
    pieces = pl.cdiv(width // SLICES, LANES)
    smem = pl.BlockSpec(memory_space=pltpu.SMEM)
    vmem = pl.BlockSpec(memory_space=pltpu.VMEM)
    return pl.pallas_call(
        peak_kernel,
        out_shape=[
            pltpu.VMEM((layers * SLICES, CAP, LANES), jnp.bfloat16),
            pltpu.VMEM((n_select, tokens, width), jnp.bfloat16),
            pltpu.SMEM((layers * CAP,), jnp.int32),
            pltpu.SMEM((layers,), jnp.int32),
        ],
        in_specs=[smem, smem, smem, pl.BlockSpec(memory_space=pltpu.HBM)],
        out_specs=[vmem, vmem, smem, smem],
        scratch_shapes=[
            pltpu.VMEM((layers, 8, width), jnp.float32),
            pltpu.VMEM((SLICES * pieces, layers, LANES), jnp.float32),
            pltpu.SemaphoreType.DMA((n_select,)),
        ],
        compiler_params=pltpu.CompilerParams(vmem_limit_bytes=2 * VMEM_LIMIT),
        cost_estimate=pl.CostEstimate(flops=20_000_000, bytes_accessed=2_500_000, transcendentals=0),
        name="peaks",
    )(sel_index, sel_layer, counts, block_pool)


def lay_out_kernel(slots, filled, held, built, spread, dirty):
    layers = filled.shape[0]
    tokens, width = held.shape[1:]
    half = width // SLICES
    tiles = spread.shape[0]
    pitch = spread.shape[1] // (CAP + 1)
    group = QUAD * half
    dirty[0] = CAP

    def build(layer, carry):
        held_slots = filled[layer]

        @pl.when(held_slots == 0)
        def _():
            built[pl.ds(SLICES * layer, SLICES), :, : tokens * half] = jnp.zeros(
                (SLICES, CAP, tokens * half), built.dtype
            )

        @pl.when(held_slots > 0)
        def _():
            def place(c, carry):
                values = held[slots[layer * CAP + c]].astype(jnp.float32)
                rows = pl.ds(c * pitch, tokens)
                for i in range(tiles):
                    lanes = min(LANES, width - i * LANES)
                    spread[i, rows, :lanes] = values[:, i * LANES : i * LANES + lanes]
                return carry

            lax.fori_loop(0, held_slots, place, 0)

            def blank(c, carry):
                for i in range(tiles):
                    spread[i, pl.ds(c * pitch, tokens), :] = jnp.zeros((tokens, LANES), jnp.float32)
                return carry

            lax.fori_loop(held_slots, dirty[0], blank, 0)
            dirty[0] = held_slots

            def four_tokens(u, carry):
                rows = [
                    [spread[i, pl.ds(QUAD * u + q, CAP, stride=pitch), :] for i in range(tiles)] for q in range(QUAD)
                ]
                for h in range(SLICES):
                    for i, tile in enumerate(end_to_end(rows, half, h * half)):
                        where = pl.ds(pl.multiple_of(u * group + i * LANES, LANES), LANES)
                        built[SLICES * layer + h, :, where] = tile.astype(jnp.bfloat16)
                return carry

            lax.fori_loop(0, tokens // QUAD, four_tokens, 0, unroll=tokens // QUAD)

        return carry

    lax.fori_loop(0, layers, build, 0)


def lay_out(held, slots, filled):
    layers = filled.shape[0]
    _, tokens, width = held.shape
    flat = tokens * (width // SLICES)
    pitch = tokens + 1
    smem = pl.BlockSpec(memory_space=pltpu.SMEM)
    vmem = pl.BlockSpec(memory_space=pltpu.VMEM)
    return pl.pallas_call(
        lay_out_kernel,
        out_shape=pltpu.VMEM((layers * SLICES, CAP, flat + LANES), jnp.bfloat16),
        in_specs=[smem, smem, vmem],
        out_specs=vmem,
        scratch_shapes=[
            pltpu.VMEM((pl.cdiv(width, LANES), (CAP + 1) * pitch, LANES), jnp.float32),
            pltpu.SMEM((1,), jnp.int32),
        ],
        compiler_params=pltpu.CompilerParams(vmem_limit_bytes=VMEM_LIMIT),
        cost_estimate=pl.CostEstimate(flops=200_000_000, bytes_accessed=12_000_000, transcendentals=0),
        name="lay_out",
    )(slots, filled, held)


BATCH = 2


def encode_kernel(raw_ref, codes_ref, steps_ref, error_ref, inverse, codes, out_sems):
    sources = raw_ref.shape[0]
    first, cap, flat = codes.shape
    lanes = inverse.shape[1]
    half = lanes // QUAD
    tiles = lanes // LANES
    batches = sources // BATCH

    def give(b):
        here = pl.ds(b * BATCH, BATCH)
        return pltpu.make_async_copy(codes.at[here], codes_ref.at[here], out_sems.at[b])

    peak = jnp.max(raw_ref[:, :, flat:].astype(jnp.float32), axis=0)
    scale = headroom * jnp.maximum(peak, 1.0) / 127.0
    rows = [jnp.broadcast_to(scale[n : n + 1], (cap, LANES)) for n in range(pl.cdiv(half, LANES))]
    for n, row in enumerate(rows):
        size = min(LANES, half - n * LANES)
        steps_ref[:, n * LANES : n * LANES + size] = row[:1, :size]
    for i, tile in enumerate(end_to_end([rows] * QUAD, half, 0)):
        inverse[:, i * LANES : (i + 1) * LANES] = 1.0 / tile
    by_lane = [inverse[:, i * LANES : (i + 1) * LANES] for i in range(tiles)]

    def batch(b, totals, coding):
        def group(u, totals):
            totals = list(totals)
            for s in range(BATCH):
                for i in range(tiles):
                    at = pl.ds(pl.multiple_of(u * lanes + i * LANES, LANES), LANES)
                    exact = raw_ref[b * BATCH + s, :, at].astype(jnp.float32) * by_lane[i]
                    coded = jnp.clip(exact, -127.0, 127.0).astype(jnp.bfloat16)
                    if coding:
                        codes[b * BATCH + s, :, at] = coded
                    miss = exact - coded.astype(jnp.float32)
                    totals[i] = totals[i] + miss * miss
            return tuple(totals)

        totals = lax.fori_loop(0, flat // lanes, group, totals, unroll=flat // lanes)
        if coding:
            give(b).start()
        return totals

    totals = tuple(jnp.zeros((cap, LANES), jnp.float32) for _ in range(tiles))
    totals = lax.fori_loop(0, first // BATCH, functools.partial(batch, coding=True), totals)
    totals = lax.fori_loop(first // BATCH, batches, functools.partial(batch, coding=False), totals)
    whole = jnp.concatenate([jnp.sum(t, axis=0, keepdims=True) for t in totals], axis=1)
    error = whole[:, :half]
    for q in range(1, QUAD):
        error = error + whole[:, q * half : (q + 1) * half]
    error_ref[...] = error
    for b in range(first // BATCH):
        give(b).wait()


def encode(raw, half, first):
    sources, cap, size = raw.shape
    flat = size - LANES
    vmem = pl.BlockSpec(memory_space=pltpu.VMEM)
    return pl.pallas_call(
        encode_kernel,
        out_shape=[
            jax.ShapeDtypeStruct((sources, cap, flat), jnp.bfloat16),
            jax.ShapeDtypeStruct((1, half), jnp.float32),
            pltpu.VMEM((1, half), jnp.float32),
            pltpu.VMEM((cap, QUAD * half), jnp.float32),
        ],
        in_specs=[vmem],
        out_specs=[pl.BlockSpec(memory_space=pltpu.HBM), vmem, vmem, vmem],
        scratch_shapes=[
            pltpu.VMEM((first, cap, flat), jnp.bfloat16),
            pltpu.SemaphoreType.DMA((first // BATCH,)),
        ],
        compiler_params=pltpu.CompilerParams(vmem_limit_bytes=VMEM_LIMIT),
        cost_estimate=pl.CostEstimate(flops=80_000_000, bytes_accessed=19_000_000, transcendentals=0),
        name="encode",
    )(raw)


def encode_rest_kernel(raw_ref, inverse, _, codes_ref, codes, out_sems):
    count, _, flat = codes.shape
    first = raw_ref.shape[0] - count
    lanes = inverse.shape[1]
    by_lane = [inverse[:, i : i + LANES] for i in range(0, lanes, LANES)]

    def give(b):
        here = pl.ds(b * BATCH, BATCH)
        return pltpu.make_async_copy(codes.at[here], codes_ref.at[pl.ds(first + b * BATCH, BATCH)], out_sems.at[b])

    def batch(b, carry):
        for s in range(BATCH):
            for i in range(flat // LANES):
                at = slice(i * LANES, (i + 1) * LANES)
                exact = raw_ref[first + b * BATCH + s, :, at].astype(jnp.float32) * by_lane[i % len(by_lane)]
                codes[b * BATCH + s, :, at] = jnp.clip(exact, -127.0, 127.0).astype(jnp.bfloat16)
        give(b).start()
        return carry

    lax.fori_loop(0, count // BATCH, batch, 0)
    for b in range(count // BATCH):
        give(b).wait()


def encode_rest(raw, inverse, codes, first):
    rest = raw.shape[0] - first
    vmem = pl.BlockSpec(memory_space=pltpu.VMEM)
    hbm = pl.BlockSpec(memory_space=pltpu.HBM)
    return pl.pallas_call(
        encode_rest_kernel,
        out_shape=jax.ShapeDtypeStruct(codes.shape, codes.dtype),
        in_specs=[vmem, vmem, hbm],
        out_specs=hbm,
        scratch_shapes=[
            pltpu.VMEM((rest, *codes.shape[1:]), codes.dtype),
            pltpu.SemaphoreType.DMA((rest // BATCH,)),
        ],
        input_output_aliases={2: 0},
        compiler_params=pltpu.CompilerParams(vmem_limit_bytes=VMEM_LIMIT),
        cost_estimate=pl.CostEstimate(flops=200_000_000, bytes_accessed=5_000_000, transcendentals=0),
        name="encode_rest",
    )(raw, inverse, codes)


def from_others(x, axis):
    count = lax.axis_size(axis)
    return [lax.ppermute(x, axis, [(r, (r + k) % count) for r in range(count)]) for k in range(1, count)]


def body(block_pool, sel_index, sel_layer, counts):
    own_count = lax.axis_size("own")
    rep_count = lax.axis_size("rep")
    layers = own_count // SLICES
    tokens, width = block_pool.shape[1:]
    half = width // SLICES
    peak, *found = local_peaks(block_pool, sel_index, sel_layer, counts, layers)
    others = from_others(peak, "rep")
    sent = lay_out(*found)
    peak = functools.reduce(jnp.maximum, others, peak)
    sent = lax.dynamic_update_slice(sent, peak, (0, 0, tokens * half))
    arrived = lax.all_to_all(sent, "own", split_axis=0, concat_axis=0, tiled=True)

    first = own_count * 7 // 8
    codes, steps, error, inverse = encode(arrived, half, first)
    others = from_others(error, "rep")
    codes = encode_rest(arrived, inverse, codes, first)
    error = functools.reduce(jnp.add, others, error)
    denominator = float(own_count * rep_count * CAP * tokens)
    return codes[None, None], steps, error / denominator


def solution(mesh):
    return jax.shard_map(
        body,
        mesh=mesh,
        in_specs=(
            P(("own", "rep"), None, None),
            P(("own", "rep")),
            P(("own", "rep")),
            P(("own", "rep")),
        ),
        out_specs=(P("own", "rep", None, None, None), P("own", None), P("own", None)),
        check_vma=False,
    )
```

```python
import functools
import jax
import jax.numpy as jnp
from jax import lax
from jax.experimental import pallas as pl
from jax.experimental.pallas import tpu as pltpu
from jax.sharding import PartitionSpec as P

SLICES = 2
CAP = 8
LANES = 128
QUAD = 4
headroom = 0.5
VMEM_LIMIT = 30 * 2**20


def end_to_end(rows, width, start):
    lane = lax.broadcasted_iota(jnp.int32, rows[0][0].shape, 1)
    turned, out = {}, []
    for i in range(len(rows) * width // LANES):
        whole, at = None, 0
        while at < LANES:
            flat = i * LANES + at
            q = flat // width
            source = flat - q * width + start
            j = source // LANES
            run = min(LANES - source % LANES, (q + 1) * width - flat, LANES - at)
            if (q, j) not in turned:
                shift = (at - source) % LANES
                turned[q, j] = pltpu.roll(rows[q][j], shift, 1) if shift else rows[q][j]
            piece = turned[q, j]
            whole = piece if whole is None else jnp.where(lane >= at, piece, whole)
            at += run
        out.append(whole)
    return out


def peak_kernel(index_ref, layer_ref, count_ref, pool_ref, out_ref, held, slots, filled, acc, top, sems):
    live = count_ref[0]
    tokens, width = held.shape[1:]
    layers = acc.shape[0]
    half = width // SLICES
    pieces = top.shape[0] // SLICES

    def fetch(j):
        return pltpu.make_async_copy(pool_ref.at[index_ref[j]], held.at[j], sems.at[j])

    for layer in range(layers):
        filled[layer] = 0

    def start(j, carry):
        fetch(j).start()
        layer = layer_ref[j]
        at = filled[layer]
        slots[layer * CAP + at] = j
        filled[layer] = at + 1
        return carry

    lax.fori_loop(0, live, start, 0)
    acc[...] = jnp.zeros_like(acc)
    top[...] = jnp.zeros_like(top)

    def wait(j, carry):
        fetch(j).wait()
        layer = layer_ref[j]
        values = jnp.abs(held[j])
        rows = tokens
        while rows > 16:
            rows //= 2
            values = jnp.maximum(values[:rows], values[rows:])
        values = values.astype(jnp.float32)
        acc[layer] = jnp.maximum(acc[layer], jnp.maximum(values[:8], values[8:]))
        return carry

    lax.fori_loop(0, live, wait, 0)
    whole = jnp.max(acc[...], axis=1)
    for h in range(SLICES):
        for n in range(pieces):
            lanes = min(LANES, half - n * LANES)
            at = h * half + n * LANES
            top[h * pieces + n, :, :lanes] = whole[:, at : at + lanes]
    row = lax.broadcasted_iota(jnp.int32, (CAP, LANES), 0)

    def tiles(layer, carry):
        for h in range(SLICES):
            tile = jnp.zeros((CAP, LANES), jnp.float32)
            for n in range(pieces):
                one = jnp.broadcast_to(top[h * pieces + n, pl.ds(layer, 1), :], (CAP, LANES))
                tile = jnp.where(row == n, one, tile)
            out_ref[layer * SLICES + h] = tile.astype(jnp.bfloat16)
        return carry

    lax.fori_loop(0, layers, tiles, 0, unroll=4)


def local_peaks(block_pool, sel_index, sel_layer, counts, layers):
    n_select = sel_index.shape[0]
    tokens, width = block_pool.shape[1:]
    pieces = pl.cdiv(width // SLICES, LANES)
    smem = pl.BlockSpec(memory_space=pltpu.SMEM)
    vmem = pl.BlockSpec(memory_space=pltpu.VMEM)
    return pl.pallas_call(
        peak_kernel,
        out_shape=[
            pltpu.VMEM((layers * SLICES, CAP, LANES), jnp.bfloat16),
            pltpu.VMEM((n_select, tokens, width), jnp.bfloat16),
            pltpu.SMEM((layers * CAP,), jnp.int32),
            pltpu.SMEM((layers,), jnp.int32),
        ],
        in_specs=[smem, smem, smem, pl.BlockSpec(memory_space=pltpu.HBM)],
        out_specs=[vmem, vmem, smem, smem],
        scratch_shapes=[
            pltpu.VMEM((layers, 8, width), jnp.float32),
            pltpu.VMEM((SLICES * pieces, layers, LANES), jnp.float32),
            pltpu.SemaphoreType.DMA((n_select,)),
        ],
        compiler_params=pltpu.CompilerParams(vmem_limit_bytes=2 * VMEM_LIMIT),
        cost_estimate=pl.CostEstimate(flops=20_000_000, bytes_accessed=2_500_000, transcendentals=0),
        name="peaks",
    )(sel_index, sel_layer, counts, block_pool)


def lay_out_kernel(slots, filled, held, built, spread, dirty):
    layers = filled.shape[0]
    tokens, width = held.shape[1:]
    half = width // SLICES
    tiles = spread.shape[0]
    pitch = spread.shape[1] // (CAP + 1)
    group = QUAD * half
    dirty[0] = CAP

    def build(layer, carry):
        held_slots = filled[layer]

        @pl.when(held_slots == 0)
        def _():
            built[pl.ds(SLICES * layer, SLICES), :, : tokens * half] = jnp.zeros(
                (SLICES, CAP, tokens * half), built.dtype
            )

        @pl.when(held_slots > 0)
        def _():
            def place(c, carry):
                values = held[slots[layer * CAP + c]].astype(jnp.float32)
                rows = pl.ds(c * pitch, tokens)
                for i in range(tiles):
                    lanes = min(LANES, width - i * LANES)
                    spread[i, rows, :lanes] = values[:, i * LANES : i * LANES + lanes]
                return carry

            lax.fori_loop(0, held_slots, place, 0)

            def blank(c, carry):
                for i in range(tiles):
                    spread[i, pl.ds(c * pitch, tokens), :] = jnp.zeros((tokens, LANES), jnp.float32)
                return carry

            lax.fori_loop(held_slots, dirty[0], blank, 0)
            dirty[0] = held_slots

            def four_tokens(u, carry):
                rows = [
                    [spread[i, pl.ds(QUAD * u + q, CAP, stride=pitch), :] for i in range(tiles)] for q in range(QUAD)
                ]
                for h in range(SLICES):
                    for i, tile in enumerate(end_to_end(rows, half, h * half)):
                        where = pl.ds(pl.multiple_of(u * group + i * LANES, LANES), LANES)
                        built[SLICES * layer + h, :, where] = tile.astype(jnp.bfloat16)
                return carry

            lax.fori_loop(0, tokens // QUAD, four_tokens, 0, unroll=tokens // QUAD)

        return carry

    lax.fori_loop(0, layers, build, 0)


def lay_out(held, slots, filled):
    layers = filled.shape[0]
    _, tokens, width = held.shape
    flat = tokens * (width // SLICES)
    pitch = tokens + 1
    smem = pl.BlockSpec(memory_space=pltpu.SMEM)
    vmem = pl.BlockSpec(memory_space=pltpu.VMEM)
    return pl.pallas_call(
        lay_out_kernel,
        out_shape=pltpu.VMEM((layers * SLICES, CAP, flat + LANES), jnp.bfloat16),
        in_specs=[smem, smem, vmem],
        out_specs=vmem,
        scratch_shapes=[
            pltpu.VMEM((pl.cdiv(width, LANES), (CAP + 1) * pitch, LANES), jnp.float32),
            pltpu.SMEM((1,), jnp.int32),
        ],
        compiler_params=pltpu.CompilerParams(vmem_limit_bytes=VMEM_LIMIT),
        cost_estimate=pl.CostEstimate(flops=200_000_000, bytes_accessed=12_000_000, transcendentals=0),
        name="lay_out",
    )(slots, filled, held)


BATCH = 2


def encode_kernel(raw_ref, codes_ref, steps_ref, error_ref, codes, inverse, out_sems):
    sources, cap, flat = codes.shape
    lanes = inverse.shape[1]
    half = lanes // QUAD
    tiles = lanes // LANES
    batches = sources // BATCH

    def give(b):
        here = pl.ds(b * BATCH, BATCH)
        return pltpu.make_async_copy(codes.at[here], codes_ref.at[here], out_sems.at[b])

    peak = jnp.max(raw_ref[:, :, flat:].astype(jnp.float32), axis=0)
    scale = headroom * jnp.maximum(peak, 1.0) / 127.0
    rows = [jnp.broadcast_to(scale[n : n + 1], (cap, LANES)) for n in range(pl.cdiv(half, LANES))]
    for n, row in enumerate(rows):
        size = min(LANES, half - n * LANES)
        steps_ref[:, n * LANES : n * LANES + size] = row[:1, :size]
    for i, tile in enumerate(end_to_end([rows] * QUAD, half, 0)):
        inverse[:, i * LANES : (i + 1) * LANES] = 1.0 / tile
    by_lane = [inverse[:, i * LANES : (i + 1) * LANES] for i in range(tiles)]

    def batch(b, totals):
        def group(u, totals):
            totals = list(totals)
            for s in range(BATCH):
                for i in range(tiles):
                    at = pl.ds(pl.multiple_of(u * lanes + i * LANES, LANES), LANES)
                    exact = raw_ref[b * BATCH + s, :, at].astype(jnp.float32) * by_lane[i]
                    coded = jnp.clip(exact, -127.0, 127.0).astype(jnp.bfloat16)
                    codes[b * BATCH + s, :, at] = coded
                    miss = exact - coded.astype(jnp.float32)
                    totals[i] = totals[i] + miss * miss
            return tuple(totals)

        totals = lax.fori_loop(0, flat // lanes, group, totals, unroll=flat // lanes)
        give(b).start()
        return totals

    totals = lax.fori_loop(
        0, batches, batch, tuple(jnp.zeros((cap, LANES), jnp.float32) for _ in range(tiles))
    )
    whole = jnp.concatenate([jnp.sum(t, axis=0, keepdims=True) for t in totals], axis=1)
    error = whole[:, :half]
    for q in range(1, QUAD):
        error = error + whole[:, q * half : (q + 1) * half]
    error_ref[...] = error
    for b in range(batches):
        give(b).wait()


def encode(raw, half):
    sources, cap, size = raw.shape
    flat = size - LANES
    vmem = pl.BlockSpec(memory_space=pltpu.VMEM)
    return pl.pallas_call(
        encode_kernel,
        out_shape=[
            jax.ShapeDtypeStruct((sources, cap, flat), jnp.bfloat16),
            jax.ShapeDtypeStruct((1, half), jnp.float32),
            pltpu.VMEM((1, half), jnp.float32),
        ],
        in_specs=[vmem],
        out_specs=[pl.BlockSpec(memory_space=pltpu.HBM), vmem, vmem],
        scratch_shapes=[
            pltpu.VMEM((sources, cap, flat), jnp.bfloat16),
            pltpu.VMEM((cap, QUAD * half), jnp.float32),
            pltpu.SemaphoreType.DMA((sources // BATCH,)),
        ],
        compiler_params=pltpu.CompilerParams(vmem_limit_bytes=VMEM_LIMIT),
        cost_estimate=pl.CostEstimate(flops=80_000_000, bytes_accessed=19_000_000, transcendentals=0),
        name="encode",
    )(raw)


def from_others(x, axis):
    count = lax.axis_size(axis)
    return [lax.ppermute(x, axis, [(r, (r + k) % count) for r in range(count)]) for k in range(1, count)]


def body(block_pool, sel_index, sel_layer, counts):
    own_count = lax.axis_size("own")
    rep_count = lax.axis_size("rep")
    layers = own_count // SLICES
    tokens, width = block_pool.shape[1:]
    half = width // SLICES
    peak, *found = local_peaks(block_pool, sel_index, sel_layer, counts, layers)
    others = from_others(peak, "rep")
    sent = lay_out(*found)
    peak = functools.reduce(jnp.maximum, others, peak)
    sent = lax.dynamic_update_slice(sent, peak, (0, 0, tokens * half))
    arrived = lax.all_to_all(sent, "own", split_axis=0, concat_axis=0, tiled=True)

    codes, steps, error = encode(arrived, half)
    error = functools.reduce(jnp.add, from_others(error, "rep"), error)
    denominator = float(own_count * rep_count * CAP * tokens)
    return codes[None, None], steps, error / denominator


def solution(mesh):
    return jax.shard_map(
        body,
        mesh=mesh,
        in_specs=(
            P(("own", "rep"), None, None),
            P(("own", "rep")),
            P(("own", "rep")),
            P(("own", "rep")),
        ),
        out_specs=(P("own", "rep", None, None, None), P("own", None), P("own", None)),
        check_vma=False,
    )
```
